32 devices in a mesh: real: 2 (over x), row: 16 (over z, y, core).
Axes of the slice: x: 2, y: 2, z: 4, core: 2. Of those that a mesh axis runs over, the one named last changes fastest.
Arguments:
- site_tensor: float32 [32, 2, 256, 256], P(('real', 'row')), parts along dimension 0, may hold values from -20 to 20
- left_env: float32 [32, 14, 256, 256], P(('real', 'row')), parts along dimension 0, may hold values from -10 to 10
- right_env: float32 [32, 14, 256, 256], P(('real', 'row')), parts along dimension 0, may hold values from -10 to 10
- sector_size: int32 [32], P('real'), parts along dimension 0, may hold values from 64 to 256
Outputs:
- left_out: float32 [32, 2, 256, 256], P(('real', 'row')), parts along dimension 0
- bond_out: float32 [32, 256, 256], P(('real', 'row')), parts along dimension 0
The draws below stay inside these ranges and needn't reach their ends.
There are 2 independent parts, one for each index of `real`. The reference program is written for one: setup_inputs(seed, part) draws one part's arguments, and reference() takes and returns one part's arrays. A program takes and returns all parts, laid end to end along the dimension named above; each array names one. Nothing has to cross between parts.
All inputs are finite; a program needn't handle non-finite values.
Results may differ from the reference program's by a relative error of at most 0.00005.
Values sent between devices are 32-bit elements; how exact they have to be, the bound alone decides.
A program may use at most 64 MiB of HBM per device.

```python
import jax
import jax.numpy as jnp
from jax import lax

SEC = 256
W_DN = 4
W_UP = 4
W = 14
SECTORS = 16


def sector_ramp(total_rise):
    position = jnp.arange(SECTORS, dtype=jnp.float32) / max(SECTORS - 1, 1)
    return jnp.exp(jnp.log(total_rise) * position)


def draw_site_tensor(key, part):
    key_noise, key_scale = jax.random.split(jax.random.fold_in(key, 11))
    random_part = jnp.clip(jax.random.normal(key_noise, (SECTORS, 2, SEC, SEC), jnp.float32), -6.0, 6.0)
    column_scale = jnp.exp(jnp.clip(0.2 * jax.random.normal(key_scale, (SECTORS, 2, 1, SEC), jnp.float32), -0.8, 0.8))
    ramp = jnp.sqrt(sector_ramp(3.0))
    random_part = random_part * SEC ** (-0.5)
    identity = jnp.eye(SEC, dtype=jnp.float32)
    upper_block = identity[None] + 0.35 * random_part[:, 0]
    lower_block = 0.7 * random_part[:, 1]
    return jnp.stack([upper_block, lower_block], 1) * column_scale * ramp[:, None, None, None]


def environment_noise(key):
    noise = jnp.clip(jax.random.normal(key, (SECTORS, W, SEC, SEC), jnp.float32), -6.0, 6.0)
    return noise * SEC ** (-0.5)


def draw_left_env(key, part):
    key_noise, key_field = jax.random.split(jax.random.fold_in(key, 23))
    noise = environment_noise(key_noise)
    rough = jnp.exp(jax.random.uniform(key_field, (SECTORS, SEC), jnp.float32, jnp.log(0.5), jnp.log(2.0)))
    ramp = sector_ramp(3.0)
    field = rough * ramp[:, None]
    identity = jnp.eye(SEC, dtype=jnp.float32)
    onsite = field[:, :, None] * identity[None]
    return noise.at[:, W - 1].add(onsite)


def draw_right_env(key, part):
    noise = environment_noise(jax.random.fold_in(key, 37))
    identity = jnp.eye(SEC, dtype=jnp.float32)
    return noise.at[:, W - 1].add(identity[None])


def with_ends(values, own_key, least, high):
    dims = values.shape
    index_at = [jax.random.randint(jax.random.fold_in(own_key, axis), (), 0, dims[axis]) for axis in range(len(dims))]
    values = values.at[tuple(index_at)].set(least)
    longest = dims.index(max(dims))
    index_at[longest] = (index_at[longest] + 1) % dims[longest]
    return values.at[tuple(index_at)].set(high)


def setup_inputs(seed: int = 0, part: int = 0) -> dict:
    seeds = jax.random.split(jax.random.key(seed), 5)
    part_keys = jax.random.split(jax.random.fold_in(seeds[4], part), 5)
    site_tensor = draw_site_tensor(jax.random.fold_in(jax.random.fold_in(seeds[4], part), 71), part)
    left_env = draw_left_env(jax.random.fold_in(jax.random.fold_in(seeds[4], part), 71), part)
    right_env = draw_right_env(jax.random.fold_in(jax.random.fold_in(seeds[4], part), 71), part)
    sector_size = with_ends(jax.random.randint(part_keys[3], (SECTORS,), SEC // 4, SEC + 1), jax.random.fold_in(part_keys[3], 1), SEC // 4, SEC).astype(jnp.int32)
    return {"site_tensor": site_tensor, "left_env": left_env, "right_env": right_env, "sector_size": sector_size}


highest = lax.Precision.HIGHEST
time_step = 0.15

def solve_rows(factor, stacked):
    return jax.scipy.linalg.solve_triangular(factor, stacked.T, lower=True).T

def apply_bond(operand, left_env, right_env, mask_pair):
    products = jnp.einsum('sik,sakl->sail', operand, right_env, precision=highest)
    empty_block = jnp.zeros_like(products[:1])
    down_terms = jnp.concatenate([empty_block[:, :W_DN], products[:-1, :W_DN]], 0)
    upper_terms = jnp.concatenate([products[1:, W_DN:W_DN + W_UP], empty_block[:, W_DN:W_DN + W_UP]], 0)
    combined = jnp.concatenate([down_terms, upper_terms, products[:, W_DN + W_UP:]], 1)
    return jnp.einsum('saij,sajl->sil', left_env, combined, precision=highest) * mask_pair

def reference(site_tensor, left_env, right_env, sector_size):
    live_mask = (jnp.arange(SEC, dtype=jnp.int32)[None, :] < sector_size[:, None]).astype(jnp.float32)
    row_mask = live_mask[:, :, None]
    col_mask = live_mask[:, None, :]
    mask_pair = row_mask * col_mask
    upper_block = site_tensor[:, 0] * mask_pair
    lower_source = site_tensor[:, 1] * row_mask
    lower_block = jnp.concatenate([jnp.zeros_like(lower_source[:1]), lower_source[:-1]], 0) * col_mask
    stacked = jnp.concatenate([upper_block, lower_block], 1)
    identity = jnp.eye(SEC, dtype=jnp.float32)
    gram_matrix = jnp.einsum('sij,sik->sjk', stacked, stacked, precision=highest) + identity[None] * (1.0 - live_mask)[:, None, :]
    factor = jnp.linalg.cholesky(gram_matrix)
    orthonormal = jax.vmap(solve_rows)(factor, stacked)
    moved_back = jnp.concatenate([orthonormal[1:, SEC:], jnp.zeros_like(orthonormal[:1, SEC:])], 0)
    left_out = jnp.stack([orthonormal[:, :SEC], moved_back], 1)
    bond_matrix = jnp.swapaxes(factor, 1, 2) * mask_pair
    start_norm = jnp.sum(bond_matrix * bond_matrix)
    applied = apply_bond(bond_matrix, left_env, right_env, mask_pair)
    energy = jnp.sum(bond_matrix * applied) / start_norm
    shifted = applied - energy * bond_matrix
    second = apply_bond(shifted, left_env, right_env, mask_pair) - energy * shifted
    evolved = bond_matrix + time_step * shifted + 0.5 * time_step * time_step * second
    final_norm = jnp.sum(evolved * evolved)
    return (left_out, evolved * jnp.sqrt(start_norm / final_norm))
```

```python
import jax
import jax.numpy as jnp
from jax import lax
from jax.experimental import pallas as pl
from jax.experimental.pallas import tpu as pltpu
from jax.sharding import PartitionSpec as P

SIDE = 4
EARLY = 3
PANEL = 16
TAU = 0.15
highest = lax.Precision.HIGHEST
f32 = jnp.float32
bf16 = jnp.bfloat16
MESH = pl.DeviceIdType.MESH


def dot(a, b):
    return jnp.dot(a, b, preferred_element_type=f32)


def exact_dot(a, b, dims):
    return lax.dot_general(a, b, (dims, ((), ())), precision=highest, preferred_element_type=f32)


def split_2(value):
    high = value.astype(bf16)
    return high, (value - high.astype(f32)).astype(bf16)


def split_3(value):
    high = value.astype(bf16)
    rest = value - high.astype(f32)
    middle = rest.astype(bf16)
    return high, middle, (rest - middle.astype(f32)).astype(bf16)


def store_split(pair_ref, index, value):
    high, low = split_2(value)
    pair_ref[0, index] = high
    pair_ref[1, index] = low


def row_sum(value):
    rows, columns = value.shape
    summed = jnp.sum(value.reshape(rows // 8, 8, columns), axis=0)
    total = summed[:, :128]
    for start in range(128, columns, 128):
        total = total + summed[:, start : start + 128]
    return jnp.sum(total, axis=0, keepdims=True)


def square(top_left, top_right, bottom_left, bottom_right):
    top = jnp.concatenate([top_left, top_right], 1)
    return jnp.concatenate([top, jnp.concatenate([bottom_left, bottom_right], 1)], 0)


def panel_step(p, lo, hi, states, aug_ref, out_ref):
    base = pl.multiple_of(p * PANEL, PANEL)
    row_id = lax.broadcasted_iota(jnp.int32, (PANEL, 128), 0)
    offset = lax.rem(p * PANEL, 128)
    diag = aug_ref[pl.ds(base, PANEL), lo : lo + 128]
    diag = pltpu.roll(diag, lax.rem(128 - offset, 128), 1)
    columns = [jnp.broadcast_to(diag[:, r : r + 1], (PANEL, 128)) for r in range(PANEL)]
    tiles = [aug_ref[pl.ds(base, PANEL), t : t + 128] for t in range(lo, hi, 128)]
    scale = jnp.zeros((PANEL, 128), f32)
    for r in range(PANEL):
        inverse = lax.rsqrt(columns[r][r : r + 1, :])
        scale = jnp.where(row_id == r, inverse, scale)
        multiplier = columns[r] * inverse
        below = jnp.where(row_id > r, multiplier, 0.0)
        for s in range(r + 1, PANEL):
            columns[s] = columns[s] - below * multiplier[s : s + 1, :]
        if r < PANEL - 1:
            tiles = [tile - below * (tile[r : r + 1, :] * inverse) for tile in tiles]
    tiles = [tile * scale for tile in tiles]
    for t, tile in zip(range(lo, hi, 128), tiles):
        out_ref[pl.ds(base, PANEL), t : t + 128] = tile
    panel = jnp.concatenate(tiles, 1)
    q1, q2, q3 = split_3(panel)
    p1, p2, p3 = (q[:, : states - lo] for q in (q1, q2, q3))
    left = jnp.concatenate([p1, p1, p2, p2, p1, p3], 0)
    right = jnp.concatenate([q1, q2, q1, q2, q3, q1], 0)
    update = lax.dot_general(left, right, (((0,), (0,)), ((), ())), preferred_element_type=f32)
    aug_ref[lo:states, lo:hi] -= update


def kernel(
    size_ref, site_hbm, left_hbm, right_hbm,
    left_out, bond_out,
    site, gram_own, gram_in, left_f, right_f, left_s, right_s, aug, fac, bond_own, bond_in, inv_own, inv_in,
    bond, applied, applied_in, acc, field_s, red_in, red_own, local_sem, send_sem, recv_sem, red_send, red_recv,
):
    count = lax.axis_size("row")
    me = lax.axis_index("row")
    states = site.shape[-1]
    half = states // 2
    channels = left_f.shape[0]
    moved = 2 * SIDE
    not_first, not_last = me > 0, me < count - 1
    to_right, to_left = jnp.minimum(me + 1, count - 1), jnp.maximum(me - 1, 0)

    loads = [
        pltpu.make_async_copy(site_hbm.at[0], site, local_sem.at[0]),
        pltpu.make_async_copy(left_hbm.at[0], left_f, local_sem.at[1]),
        pltpu.make_async_copy(right_hbm.at[0, moved:], right_f.at[moved:], local_sem.at[2]),
    ]
    for load in loads:
        load.start()

    barrier = pltpu.get_barrier_semaphore()
    for step in range(1, count):
        peer = lax.rem(me + step, count)
        pl.semaphore_signal(barrier, inc=1, device_id={"row": peer}, device_id_type=MESH)

    def remote(source, target, slot, peer):
        return pltpu.make_async_remote_copy(
            src_ref=source, dst_ref=target, send_sem=send_sem.at[slot], recv_sem=recv_sem.at[slot],
            device_id={"row": peer}, device_id_type=MESH,
        )

    gram_slot, bond_slot, applied_slot, inv_slot = moved, moved + 1, moved + 3, moved + 5
    send_gram = remote(gram_own, gram_in, gram_slot, to_right)
    send_down = [remote(right_hbm.at[0, a], right_f.at[a], a, to_right) for a in range(SIDE)]
    send_up = [remote(right_hbm.at[0, a], right_f.at[a], a, to_left) for a in range(SIDE, moved)]
    send_bond = [remote(bond_own, bond_in.at[s], bond_slot + s, (to_right, to_left)[s]) for s in range(2)]
    send_applied = [remote(applied, applied_in.at[s], applied_slot + s, (to_right, to_left)[s]) for s in range(2)]
    send_inv = remote(inv_own, inv_in, inv_slot, to_left)

    size = size_ref[me]
    size_before = size_ref[to_left]
    size_after = size_ref[to_right]
    row = lax.broadcasted_iota(jnp.int32, (states, states), 0)
    column = lax.broadcasted_iota(jnp.int32, (states, states), 1)
    block_row, block_column = row[:half, :half], column[:half, :half]
    on_diagonal = block_row == block_column
    live_pair = (row < size) & (column < size)

    @pl.when(me == 0)
    def _():
        gram_in[...] = jnp.zeros_like(gram_in)
        right_f[:SIDE] = jnp.zeros((SIDE, states, states), f32)
        bond_in[0] = jnp.zeros(bond_in.shape[1:], f32)
        applied_in[0] = jnp.zeros((states, states), f32)

    @pl.when(me == count - 1)
    def _():
        right_f[SIDE:moved] = jnp.zeros((SIDE, states, states), f32)
        bond_in[1] = jnp.zeros(bond_in.shape[1:], f32)
        applied_in[1] = jnp.zeros((states, states), f32)
        inv_in[...] = jnp.zeros_like(inv_in)

    def diagonal_rows(block):
        values = jnp.sum(jnp.where(on_diagonal, block, 0.0), axis=0, keepdims=True)
        return jnp.broadcast_to(values, (8, half))

    def store_packed(packed_ref, block, right_block, diagonal):
        packed_ref[:half, :half] = block
        packed_ref[:half, half:] = right_block
        packed_ref[half:, :half] = diagonal
        packed_ref[half:, half:] = diagonal

    loads[0].wait()
    gram_dims = ((0,), (0,))
    outer = jnp.where((row < size) & (column < size_after), site[1], 0.0)
    gram = exact_dot(outer, outer, gram_dims)
    store_packed(
        gram_own, jnp.where(block_column >= block_row, gram[:half, :half], gram[half:, half:]),
        gram[:half, half:], diagonal_rows(gram[half:, half:]),
    )
    pl.semaphore_wait(barrier, count - 1)

    @pl.when(not_last)
    def _():
        send_gram.start()

    upper = jnp.where(live_pair, site[0], 0.0)
    site[0] = upper
    gram = exact_dot(upper, upper, gram_dims)
    gram = gram + jnp.where((row == column) & (row >= size), 1.0, 0.0)
    aug[:, states:] = jnp.where(row == column, 1.0, 0.0).astype(f32)
    fac[...] = jnp.zeros_like(fac)

    @pl.when(not_last)
    def _():
        send_gram.wait_send()
        for one in send_down[:EARLY]:
            one.start()


    @pl.when(not_first)
    def _():
        send_gram.wait_recv()
        for one in send_up[:EARLY]:
            one.start()

    block = gram_in[:half, :half]
    mirrored = block.T
    top_left = jnp.where(block_column >= block_row, block, mirrored)
    bottom_right = jnp.where(block_column < block_row, block, jnp.where(on_diagonal, gram_in[half : half + 1, :half], mirrored))
    aug[:half, :half] = gram[:half, :half] + top_left
    aug[:half, half:states] = gram[:half, half:] + gram_in[:half, half:]
    aug[half:, :half] = gram[half:, :half]
    aug[half:, half:states] = gram[half:, half:] + bottom_right
    loads[1].wait()
    loads[2].wait()

    halves = half // PANEL

    def first_half(p, carry):
        panel_step(p, 0, states + half, states, aug, fac)
        store_split(left_s, p, left_f[p])
        return carry

    def second_half(p, carry):
        panel_step(p, half, 2 * states, states, aug, fac)
        other = jnp.minimum(p, channels - 1)
        store_split(left_s, other, left_f[other])
        mine = jnp.minimum(p - halves + moved, channels - 1)
        store_split(right_s, mine, right_f[mine])
        return carry

    lax.fori_loop(0, halves, first_half, 0)
    lax.fori_loop(halves, 2 * halves, second_half, 0)

    bottom_right = fac[half:, half:states]
    store_packed(
        bond_own, jnp.where(block_column >= block_row, fac[:half, :half], bottom_right.T),
        fac[:half, half:states], diagonal_rows(bottom_right),
    )

    @pl.when(not_last)
    def _():
        for one in [send_bond[0]] + send_down[EARLY:]:
            one.start()

    @pl.when(not_first)
    def _():
        for one in [send_bond[1]] + send_up[EARLY:]:
            one.start()

    bond[...] = jnp.where(live_pair & (column >= row), fac[:, :states], 0.0)

    def put_field(which, value):
        field_s[which, 0], field_s[which, 1] = split_2(value)

    def add_terms(total, which, a):
        high, low_part = field_s[which, 0], field_s[which, 1]
        r_high, r_low = right_s[0, a], right_s[1, a]
        l_high, l_low = left_s[0, a], left_s[1, a]
        middle = dot(high, r_high) + dot(high, r_low) + dot(low_part, r_high)
        m_high, m_low = split_2(middle)
        return total + dot(l_high, m_high) + dot(l_high, m_low) + dot(l_low, m_high)

    def add_range(which, start, amount):
        group = 2 if amount % 2 == 0 else 1

        def some(g, carry):
            total = acc[...]
            for k in range(group):
                total = add_terms(total, which, start + g * group + k)
            acc[...] = total
            return carry

        lax.fori_loop(0, amount // group, some, 0)

    near = 1 - lax.rem(me, 2)
    has_side = [jnp.where(s == 0, not_first, not_last) for s in (near, 1 - near)]
    sides = list(zip((near, 1 - near), has_side))

    acc[...] = jnp.zeros_like(acc)
    put_field(0, bond[...])
    add_range(0, moved, channels - moved)
    inverse = jnp.where(column <= row, fac[:, states:], 0.0)
    turned = ((1,), (1,))
    left_out[0] = exact_dot(site[0], inverse, turned)
    inv_own[:, :half] = jnp.where(block_column < block_row, inverse[:half, :half], inverse[half:, half:].T)
    inv_own[:, half:] = inverse[half:, :half]

    for order, (side, there) in enumerate(sides):

        @pl.when(there)
        def _():
            remote(bond_own, bond_in.at[side], bond_slot + side, to_right).wait_recv()

        limit = jnp.where(side == 0, size_before, size_after)
        block = bond_in[side, :half, :half]
        top_left = jnp.where(block_column >= block_row, block, 0.0)
        bottom_right = jnp.where(block_column > block_row, block.T, jnp.where(on_diagonal, bond_in[side, half : half + 1, :half], 0.0))
        field = square(top_left, bond_in[side, :half, half:], jnp.zeros((half, half), f32), bottom_right)
        put_field(1 + side, jnp.where((row < limit) & (column < limit), field, 0.0))

        def side_channel(k, carry, side=side, there=there):
            a = side * SIDE + k

            @pl.when(there)
            def _():
                remote(applied, right_f.at[a], a, to_right).wait_recv()

            store_split(right_s, a, right_f[a])
            acc[...] = add_terms(acc[...], 1 + side, a)
            return carry

        lax.fori_loop(0, EARLY, side_channel, 0)
        lax.fori_loop(EARLY, SIDE, side_channel, 0)

    def reductions(t):
        for step in range(1, count):
            peer = lax.rem(me + step, count)
            yield pltpu.make_async_remote_copy(
                src_ref=red_own.at[t], dst_ref=red_in.at[t, step],
                send_sem=red_send.at[t, step], recv_sem=red_recv.at[t, step],
                device_id={"row": peer}, device_id_type=MESH,
            )

    applied[...] = jnp.where(live_pair, acc[...], 0.0)

    @pl.when(not_last)
    def _():
        send_applied[0].start()

    @pl.when(not_first)
    def _():
        send_applied[1].start()
        send_inv.start()

    red_own[0, :1] = row_sum(bond[...] * bond[...])
    red_own[0, 1:] = row_sum(bond[...] * applied[...])
    first_sums = list(reductions(0))
    for one in first_sums:
        one.start()

    acc[...] = jnp.zeros_like(acc)
    put_field(0, applied[...])
    add_range(0, moved, channels - moved)

    for order, (side, there) in enumerate(sides):

        @pl.when(there)
        def _():
            remote(applied, applied_in.at[side], applied_slot + side, to_right).wait_recv()

        put_field(1 + side, applied_in[side])
        add_range(1 + side, side * SIDE, SIDE)

    def collect(t, copies):
        total = red_own[t]
        for step, one in enumerate(copies, 1):
            one.wait_recv()
            total = total + red_in[t, step]
        return jnp.sum(total, axis=1, keepdims=True)

    total = collect(0, first_sums)
    start_norm = total[:1]
    energy = total[1:] / start_norm
    shifted = applied[...] - energy * bond[...]
    second = jnp.where(live_pair, acc[...], 0.0) - energy * applied[...] - energy * shifted
    acc[...] = bond[...] + TAU * shifted + (0.5 * TAU * TAU) * second
    red_own[1, :1] = row_sum(acc[...] * acc[...])
    red_own[1, 1:] = jnp.zeros((1, 128), f32)
    second_sums = list(reductions(1))
    for one in second_sums:
        one.start()


    @pl.when(not_last)
    def _():
        send_inv.wait_recv()

    block = inv_in[:, :half]
    near_block, near_low = bond_in[1, :half, :half], bond_in[1, half : half + 1, :half]
    zeros = jnp.zeros((half, half), f32)
    top_left = jnp.where(block_column < block_row, block, jnp.where(on_diagonal, 1.0 / near_block, 0.0))
    bottom_right = jnp.where(block_column < block_row, block.T, jnp.where(on_diagonal, 1.0 / near_low, 0.0))
    outer = jnp.where((row < size) & (column < size_after), site[1], 0.0)
    outer = exact_dot(outer, square(top_left, zeros, inv_in[:, half:], bottom_right), turned)
    left_out[1] = jnp.where(not_last, outer, 0.0)

    @pl.when(not_last)
    def _():
        for one in send_down + [send_bond[0], send_applied[0]]:
            one.wait_send()

    @pl.when(not_first)
    def _():
        for one in send_up + [send_bond[1], send_applied[1], send_inv]:
            one.wait_send()

    final_norm = collect(1, second_sums)[:1]
    bond_out[...] = acc[...] * jnp.sqrt(start_norm / final_norm)
    for one in first_sums + second_sums:
        one.wait_send()


def write_out(left, bond, left_hbm, bond_hbm, sem):
    stores = [
        pltpu.make_async_copy(left, left_hbm.at[0], sem.at[0]),
        pltpu.make_async_copy(bond, bond_hbm.at[0], sem.at[1]),
    ]
    for store in stores:
        store.start()
    for store in stores:
        store.wait()


def on_device(site_tensor, left_env, right_env, sector_size):
    states = site_tensor.shape[-1]
    channels = left_env.shape[1]
    count = lax.axis_size("row")
    block = (states, states)
    triangle = (states // 2 + 8, states)
    slots = 2 * SIDE + 6
    anywhere = pl.BlockSpec(memory_space=pl.ANY)
    inside = pl.BlockSpec(memory_space=pltpu.VMEM)
    left_out, bond_out = pl.pallas_call(
        kernel,
        out_shape=(
            pltpu.VMEM((2,) + block, f32),
            pltpu.VMEM(block, f32),
        ),
        in_specs=[pl.BlockSpec(memory_space=pltpu.SMEM)] + [pl.BlockSpec(memory_space=pltpu.HBM)] * 3,
        out_specs=(inside, inside),
        scratch_shapes=[
            pltpu.VMEM((2,) + block, f32),
            pltpu.VMEM(triangle, f32),
            pltpu.VMEM(triangle, f32),
            pltpu.VMEM((channels,) + block, f32),
            pltpu.VMEM((channels,) + block, f32),
            pltpu.VMEM((2, channels) + block, bf16),
            pltpu.VMEM((2, channels) + block, bf16),
            pltpu.VMEM((states, 2 * states), f32),
            pltpu.VMEM((states, 2 * states), f32),
            pltpu.VMEM(triangle, f32),
            pltpu.VMEM((2,) + triangle, f32),
            pltpu.VMEM((states // 2, states), f32),
            pltpu.VMEM((states // 2, states), f32),
            pltpu.VMEM(block, f32),
            pltpu.VMEM(block, f32),
            pltpu.VMEM((2,) + block, f32),
            pltpu.VMEM(block, f32),
            pltpu.VMEM((3, 2) + block, bf16),
            pltpu.VMEM((2, count, 2, 128), f32),
            pltpu.VMEM((2, 2, 128), f32),
            pltpu.SemaphoreType.DMA((3,)),
            pltpu.SemaphoreType.DMA((slots,)),
            pltpu.SemaphoreType.DMA((slots,)),
            pltpu.SemaphoreType.DMA((2, count)),
            pltpu.SemaphoreType.DMA((2, count)),
        ],
        compiler_params=pltpu.CompilerParams(
            collective_id=0, has_side_effects=True, vmem_limit_bytes=60 * 1024 * 1024
        ),
        name="bond_update",
    )(sector_size, site_tensor, left_env, right_env)
    return pl.pallas_call(
        write_out,
        out_shape=(
            jax.ShapeDtypeStruct(site_tensor.shape, f32),
            jax.ShapeDtypeStruct((1,) + block, f32),
        ),
        in_specs=[inside, inside],
        out_specs=(anywhere, anywhere),
        scratch_shapes=[pltpu.SemaphoreType.DMA((2,))],
        compiler_params=pltpu.CompilerParams(vmem_limit_bytes=4 * 1024 * 1024),
        name="write_out",
    )(left_out, bond_out)


def solution(mesh):
    placed = (
        P(("real", "row"), None, None, None),
        P(("real", "row"), None, None, None),
        P(("real", "row"), None, None, None),
        P("real"),
    )
    return jax.shard_map(
        on_device,
        mesh=mesh,
        in_specs=placed,
        out_specs=(P(("real", "row"), None, None, None), P(("real", "row"), None, None)),
        check_vma=False,
    )
```

```python
import jax
import jax.numpy as jnp
from jax import lax
from jax.experimental import pallas as pl
from jax.experimental.pallas import tpu as pltpu
from jax.sharding import PartitionSpec as P

SIDE = 4
EARLY = 3
PANEL = 16
TAU = 0.15
highest = lax.Precision.HIGHEST
f32 = jnp.float32
bf16 = jnp.bfloat16
MESH = pl.DeviceIdType.MESH


def dot(a, b):
    return jnp.dot(a, b, preferred_element_type=f32)


def exact_dot(a, b, dims):
    return lax.dot_general(a, b, (dims, ((), ())), precision=highest, preferred_element_type=f32)


def split_2(value):
    high = value.astype(bf16)
    return high, (value - high.astype(f32)).astype(bf16)


def split_3(value):
    high = value.astype(bf16)
    rest = value - high.astype(f32)
    middle = rest.astype(bf16)
    return high, middle, (rest - middle.astype(f32)).astype(bf16)


def store_split(pair_ref, index, value):
    high, low = split_2(value)
    pair_ref[0, index] = high
    pair_ref[1, index] = low


def row_sum(value):
    rows, columns = value.shape
    summed = jnp.sum(value.reshape(rows // 8, 8, columns), axis=0)
    total = summed[:, :128]
    for start in range(128, columns, 128):
        total = total + summed[:, start : start + 128]
    return jnp.sum(total, axis=0, keepdims=True)


def square(top_left, top_right, bottom_left, bottom_right):
    top = jnp.concatenate([top_left, top_right], 1)
    return jnp.concatenate([top, jnp.concatenate([bottom_left, bottom_right], 1)], 0)


def panel_step(p, lo, hi, states, aug_ref, out_ref):
    base = pl.multiple_of(p * PANEL, PANEL)
    row_id = lax.broadcasted_iota(jnp.int32, (PANEL, 128), 0)
    offset = lax.rem(p * PANEL, 128)
    diag = aug_ref[pl.ds(base, PANEL), lo : lo + 128]
    diag = pltpu.roll(diag, lax.rem(128 - offset, 128), 1)
    columns = [jnp.broadcast_to(diag[:, r : r + 1], (PANEL, 128)) for r in range(PANEL)]
    tiles = [aug_ref[pl.ds(base, PANEL), t : t + 128] for t in range(lo, hi, 128)]
    scale = jnp.zeros((PANEL, 128), f32)
    for r in range(PANEL):
        inverse = lax.rsqrt(columns[r][r : r + 1, :])
        scale = jnp.where(row_id == r, inverse, scale)
        multiplier = columns[r] * inverse
        below = jnp.where(row_id > r, multiplier, 0.0)
        for s in range(r + 1, PANEL):
            columns[s] = columns[s] - below * multiplier[s : s + 1, :]
        if r < PANEL - 1:
            tiles = [tile - below * (tile[r : r + 1, :] * inverse) for tile in tiles]
    tiles = [tile * scale for tile in tiles]
    for t, tile in zip(range(lo, hi, 128), tiles):
        out_ref[pl.ds(base, PANEL), t : t + 128] = tile
    panel = jnp.concatenate(tiles, 1)
    q1, q2, q3 = split_3(panel)
    p1, p2, p3 = (q[:, : states - lo] for q in (q1, q2, q3))
    left = jnp.concatenate([p1, p1, p2, p2, p1, p3], 0)
    right = jnp.concatenate([q1, q2, q1, q2, q3, q1], 0)
    update = lax.dot_general(left, right, (((0,), (0,)), ((), ())), preferred_element_type=f32)
    aug_ref[lo:states, lo:hi] -= update


def kernel(
    size_hbm, site_hbm, left_hbm, right_hbm,
    left_out, bond_out,
    size_ref, site, gram_own, gram_in, left_f, right_f, left_s, right_s, aug, fac, bond_own, bond_in, inv_own, inv_in,
    bond, applied, applied_in, acc, field_s, red_in, red_own, local_sem, send_sem, recv_sem, red_send, red_recv,
):
    count = lax.axis_size("row")
    me = lax.axis_index("row")
    states = site.shape[-1]
    half = states // 2
    channels = left_f.shape[0]
    moved = 2 * SIDE
    not_first, not_last = me > 0, me < count - 1
    to_right, to_left = jnp.minimum(me + 1, count - 1), jnp.maximum(me - 1, 0)

    loads = [
        pltpu.make_async_copy(site_hbm.at[0], site, local_sem.at[0]),
        pltpu.make_async_copy(left_hbm.at[0], left_f, local_sem.at[1]),
        pltpu.make_async_copy(right_hbm.at[0, moved:], right_f.at[moved:], local_sem.at[2]),
    ]
    load_size = pltpu.make_async_copy(size_hbm, size_ref, local_sem.at[3])
    load_size.start()
    for load in loads:
        load.start()

    barrier = pltpu.get_barrier_semaphore()
    for step in range(1, count):
        peer = lax.rem(me + step, count)
        pl.semaphore_signal(barrier, inc=1, device_id={"row": peer}, device_id_type=MESH)

    def remote(source, target, sent, received, peer):
        return pltpu.make_async_remote_copy(
            src_ref=source, dst_ref=target, send_sem=send_sem.at[sent], recv_sem=recv_sem.at[received],
            device_id={"row": peer}, device_id_type=MESH,
        )

    halves = [slice(0, half), slice(half, states)]
    peers = (to_right, to_left)

    def block_copy(side, k, peer):
        a = side * SIDE + k
        return remote(right_hbm.at[0, a], right_f.at[a], 1 + side, (1 if k < EARLY else 3) + side, peer)

    def blocks_sent(side):
        channels_of = pl.ds(side * SIDE, SIDE)
        return remote(right_hbm.at[0, channels_of], right_f.at[channels_of], 1 + side, 1 + side, to_right)

    def early_blocks(side):
        channels_of = pl.ds(side * SIDE, EARLY)
        return remote(right_hbm.at[0, channels_of], right_f.at[channels_of], 1 + side, 1 + side, to_right)

    def bond_copy(side, peer):
        return remote(bond_own, bond_in.at[side], 3 + side, 5 + side, peer)

    def applied_copy(side, part, peer):
        rows = halves[part]
        return remote(applied.at[rows], applied_in.at[side, rows], 5 + side, 7 + 2 * side + part, peer)

    def applied_sent(side):
        return remote(applied, applied_in.at[side], 5 + side, 7 + 2 * side, to_right)

    send_gram = remote(gram_own, gram_in, 0, 0, to_right)
    send_inv = remote(inv_own, inv_in, 7, 11, to_left)
    sends = [[block_copy(s, k, peers[s]) for k in range(SIDE)] for s in range(2)]
    send_bond = [bond_copy(s, peers[s]) for s in range(2)]
    send_applied = [[applied_copy(s, part, peers[s]) for part in range(2)] for s in range(2)]

    load_size.wait()
    size = size_ref[me]
    size_before = size_ref[to_left]
    size_after = size_ref[to_right]
    row = lax.broadcasted_iota(jnp.int32, (states, states), 0)
    column = lax.broadcasted_iota(jnp.int32, (states, states), 1)
    block_row, block_column = row[:half, :half], column[:half, :half]
    on_diagonal = block_row == block_column
    live_pair = (row < size) & (column < size)

    @pl.when(me == 0)
    def _():
        gram_in[...] = jnp.zeros_like(gram_in)
        right_f[:SIDE] = jnp.zeros((SIDE, states, states), f32)
        bond_in[0] = jnp.zeros(bond_in.shape[1:], f32)
        applied_in[0] = jnp.zeros((states, states), f32)

    @pl.when(me == count - 1)
    def _():
        right_f[SIDE:moved] = jnp.zeros((SIDE, states, states), f32)
        bond_in[1] = jnp.zeros(bond_in.shape[1:], f32)
        applied_in[1] = jnp.zeros((states, states), f32)
        inv_in[...] = jnp.zeros_like(inv_in)

    def diagonal_rows(block):
        values = jnp.sum(jnp.where(on_diagonal, block, 0.0), axis=0, keepdims=True)
        return jnp.broadcast_to(values, (8, half))

    def store_packed(packed_ref, block, right_block, diagonal):
        packed_ref[:half, :half] = block
        packed_ref[:half, half:] = right_block
        packed_ref[half:, :half] = diagonal
        packed_ref[half:, half:] = diagonal

    loads[0].wait()
    gram_dims = ((0,), (0,))
    outer = jnp.where((row < size) & (column < size_after), site[1], 0.0)
    gram = exact_dot(outer, outer, gram_dims)
    store_packed(
        gram_own, jnp.where(block_column >= block_row, gram[:half, :half], gram[half:, half:]),
        gram[:half, half:], diagonal_rows(gram[half:, half:]),
    )
    pl.semaphore_wait(barrier, count - 1)

    @pl.when(not_last)
    def _():
        send_gram.start()

    upper = jnp.where(live_pair, site[0], 0.0)
    site[0] = upper
    gram = exact_dot(upper, upper, gram_dims)
    gram = gram + jnp.where((row == column) & (row >= size), 1.0, 0.0)
    aug[:, states:] = jnp.where(row == column, 1.0, 0.0).astype(f32)
    fac[...] = jnp.zeros_like(fac)

    @pl.when(not_last)
    def _():
        send_gram.wait_send()
        for one in sends[0][:EARLY]:
            one.start()


    @pl.when(not_first)
    def _():
        send_gram.wait_recv()
        for one in sends[1][:EARLY]:
            one.start()

    block = gram_in[:half, :half]
    mirrored = block.T
    top_left = jnp.where(block_column >= block_row, block, mirrored)
    bottom_right = jnp.where(block_column < block_row, block, jnp.where(on_diagonal, gram_in[half : half + 1, :half], mirrored))
    aug[:half, :half] = gram[:half, :half] + top_left
    aug[:half, half:states] = gram[:half, half:] + gram_in[:half, half:]
    aug[half:, :half] = gram[half:, :half]
    aug[half:, half:states] = gram[half:, half:] + bottom_right
    loads[1].wait()
    loads[2].wait()

    panels = half // PANEL

    def first_half(p, carry):
        panel_step(p, 0, states + half, states, aug, fac)
        store_split(left_s, p, left_f[p])
        return carry

    def second_half(p, carry):
        panel_step(p, half, 2 * states, states, aug, fac)
        other = jnp.minimum(p, channels - 1)
        store_split(left_s, other, left_f[other])
        mine = jnp.minimum(p - panels + moved, channels - 1)
        store_split(right_s, mine, right_f[mine])
        return carry

    lax.fori_loop(0, panels, first_half, 0)
    lax.fori_loop(panels, 2 * panels, second_half, 0)

    bottom_right = fac[half:, half:states]
    store_packed(
        bond_own, jnp.where(block_column >= block_row, fac[:half, :half], bottom_right.T),
        fac[:half, half:states], diagonal_rows(bottom_right),
    )

    @pl.when(not_last)
    def _():
        for one in [send_bond[0]] + sends[0][EARLY:]:
            one.start()

    @pl.when(not_first)
    def _():
        for one in [send_bond[1]] + sends[1][EARLY:]:
            one.start()

    bond[...] = jnp.where(live_pair & (column >= row), fac[:, :states], 0.0)

    def put_field(which, value):
        field_s[which, 0], field_s[which, 1] = split_2(value)

    def middle_of(which, a, rows):
        high, low_part = field_s[which, 0, rows], field_s[which, 1, rows]
        r_high, r_low = right_s[0, a], right_s[1, a]
        return split_2(dot(high, r_high) + dot(high, r_low) + dot(low_part, r_high))

    def outside(total, l_high, l_low, m_high, m_low):
        return total + dot(l_high, m_high) + dot(l_high, m_low) + dot(l_low, m_high)

    def add_terms(total, which, a):
        m_high, m_low = middle_of(which, a, slice(None))
        return outside(total, left_s[0, a], left_s[1, a], m_high, m_low)

    def add_range(which, start, amount):
        group = 2 if amount % 2 == 0 else 1

        def some(g, carry):
            total = acc[...]
            for k in range(group):
                total = add_terms(total, which, start + g * group + k)
            acc[...] = total
            return carry

        lax.fori_loop(0, amount // group, some, 0)

    near = 1 - lax.rem(me, 2)
    has_side = [jnp.where(s == 0, not_first, not_last) for s in (near, 1 - near)]
    sides = list(zip((near, 1 - near), has_side))

    acc[...] = jnp.zeros_like(acc)
    put_field(0, bond[...])
    add_range(0, moved, channels - moved)
    inverse = jnp.where(column <= row, fac[:, states:], 0.0)
    turned = ((1,), (1,))
    left_out[0] = exact_dot(site[0], inverse, turned)
    inv_own[:, :half] = jnp.where(block_column < block_row, inverse[:half, :half], inverse[half:, half:].T)
    inv_own[:, half:] = inverse[half:, :half]

    for order, (side, there) in enumerate(sides):

        @pl.when(there)
        def _():
            bond_copy(side, to_right).wait_recv()

        limit = jnp.where(side == 0, size_before, size_after)
        block = bond_in[side, :half, :half]
        top_left = jnp.where(block_column >= block_row, block, 0.0)
        bottom_right = jnp.where(block_column > block_row, block.T, jnp.where(on_diagonal, bond_in[side, half : half + 1, :half], 0.0))
        field = square(top_left, bond_in[side, :half, half:], jnp.zeros((half, half), f32), bottom_right)
        put_field(1 + side, jnp.where((row < limit) & (column < limit), field, 0.0))

        @pl.when(there)
        def _():
            early_blocks(side).wait_recv()

        for k in range(EARLY):
            store_split(right_s, side * SIDE + k, right_f[side * SIDE + k])
        total = acc[...]
        for k in range(EARLY):
            total = add_terms(total, 1 + side, side * SIDE + k)
        acc[...] = total

        @pl.when(there)
        def _():
            block_copy(side, EARLY, to_right).wait_recv()

        last = side * SIDE + EARLY
        store_split(right_s, last, right_f[last])
        if order == 0:
            acc[...] = add_terms(acc[...], 1 + side, last)

    def reductions(t):
        for step in range(1, count):
            peer = lax.rem(me + step, count)
            yield pltpu.make_async_remote_copy(
                src_ref=red_own.at[t], dst_ref=red_in.at[t, step - 1],
                send_sem=red_send.at[t], recv_sem=red_recv.at[t],
                device_id={"row": peer}, device_id_type=MESH,
            )

    def all_reductions(t):
        return pltpu.make_async_remote_copy(
            src_ref=red_in.at[t], dst_ref=red_in.at[t], send_sem=red_send.at[t], recv_sem=red_recv.at[t],
            device_id={"row": to_right}, device_id_type=MESH,
        )

    last = (1 - near) * SIDE + EARLY
    m_high, m_low = middle_of(2 - near, last, slice(None))
    for part, rows in enumerate(halves):
        value = outside(acc[rows], left_s[0, last, rows], left_s[1, last, rows], m_high, m_low)
        applied[rows] = jnp.where(live_pair[rows], value, 0.0)
        if part == 1:
            red_own[0, :1] = row_sum(bond[...] * bond[...])
            red_own[0, 1:] = row_sum(bond[...] * applied[...])
            for one in reductions(0):
                one.start()

        @pl.when(not_last)
        def _():
            send_applied[0][part].start()

        @pl.when(not_first)
        def _():
            send_applied[1][part].start()

    acc[...] = jnp.zeros_like(acc)
    put_field(0, applied[...])
    add_range(0, moved, channels - moved)

    for order, (side, there) in enumerate(sides):
        for part, rows in enumerate(halves):

            @pl.when(there)
            def _():
                applied_copy(side, part, to_right).wait_recv()

            if order == 0 and part == 1:

                @pl.when(not_first)
                def _():
                    send_inv.start()

            which = 1 + side
            field_s[which, 0, rows], field_s[which, 1, rows] = split_2(applied_in[side, rows])
            middles = [middle_of(which, side * SIDE + k, rows) for k in range(SIDE)]
            total = acc[...]
            for k in range(0, SIDE, 2):
                pair = [side * SIDE + k, side * SIDE + k + 1]
                l_high, l_low = (jnp.concatenate([left_s[i, a, :, rows] for a in pair], 1) for i in range(2))
                m_high, m_low = (jnp.concatenate([middles[k + j][i] for j in range(2)], 0) for i in range(2))
                total = outside(total, l_high, l_low, m_high, m_low)
            acc[...] = total

    def collect(t):
        all_reductions(t).wait_recv()
        return jnp.sum(red_own[t] + jnp.sum(red_in[t], axis=0), axis=1, keepdims=True)

    total = collect(0)
    start_norm = total[:1]
    energy = total[1:] / start_norm
    shifted = applied[...] - energy * bond[...]
    second = jnp.where(live_pair, acc[...], 0.0) - energy * applied[...] - energy * shifted
    acc[...] = bond[...] + TAU * shifted + (0.5 * TAU * TAU) * second
    red_own[1, :1] = row_sum(acc[...] * acc[...])
    red_own[1, 1:] = jnp.zeros((1, 128), f32)
    for one in reductions(1):
        one.start()


    @pl.when(not_last)
    def _():
        send_inv.wait_recv()

    block = inv_in[:, :half]
    near_block, near_low = bond_in[1, :half, :half], bond_in[1, half : half + 1, :half]
    zeros = jnp.zeros((half, half), f32)
    top_left = jnp.where(block_column < block_row, block, jnp.where(on_diagonal, 1.0 / near_block, 0.0))
    bottom_right = jnp.where(block_column < block_row, block.T, jnp.where(on_diagonal, 1.0 / near_low, 0.0))
    outer = jnp.where((row < size) & (column < size_after), site[1], 0.0)
    outer = exact_dot(outer, square(top_left, zeros, inv_in[:, half:], bottom_right), turned)
    left_out[1] = jnp.where(not_last, outer, 0.0)

    @pl.when(not_last)
    def _():
        for one in [blocks_sent(0), send_bond[0], applied_sent(0)]:
            one.wait_send()

    @pl.when(not_first)
    def _():
        for one in [blocks_sent(1), send_bond[1], applied_sent(1), send_inv]:
            one.wait_send()

    final_norm = collect(1)[:1]
    bond_out[...] = acc[...] * jnp.sqrt(start_norm / final_norm)
    for t in range(2):
        all_reductions(t).wait_send()


def write_out(left, bond, left_hbm, bond_hbm, sem):
    stores = [
        pltpu.make_async_copy(left, left_hbm.at[0], sem.at[0]),
        pltpu.make_async_copy(bond, bond_hbm.at[0], sem.at[1]),
    ]
    for store in stores:
        store.start()
    for store in stores:
        store.wait()


def on_device(site_tensor, left_env, right_env, sector_size):
    states = site_tensor.shape[-1]
    channels = left_env.shape[1]
    count = lax.axis_size("row")
    block = (states, states)
    triangle = (states // 2 + 8, states)
    anywhere = pl.BlockSpec(memory_space=pl.ANY)
    inside = pl.BlockSpec(memory_space=pltpu.VMEM)
    left_out, bond_out = pl.pallas_call(
        kernel,
        out_shape=(
            pltpu.VMEM((2,) + block, f32),
            pltpu.VMEM(block, f32),
        ),
        in_specs=[pl.BlockSpec(memory_space=pltpu.HBM)] * 4,
        out_specs=(inside, inside),
        scratch_shapes=[
            pltpu.SMEM(sector_size.shape, jnp.int32),
            pltpu.VMEM((2,) + block, f32),
            pltpu.VMEM(triangle, f32),
            pltpu.VMEM(triangle, f32),
            pltpu.VMEM((channels,) + block, f32),
            pltpu.VMEM((channels,) + block, f32),
            pltpu.VMEM((2, channels) + block, bf16),
            pltpu.VMEM((2, channels) + block, bf16),
            pltpu.VMEM((states, 2 * states), f32),
            pltpu.VMEM((states, 2 * states), f32),
            pltpu.VMEM(triangle, f32),
            pltpu.VMEM((2,) + triangle, f32),
            pltpu.VMEM((states // 2, states), f32),
            pltpu.VMEM((states // 2, states), f32),
            pltpu.VMEM(block, f32),
            pltpu.VMEM(block, f32),
            pltpu.VMEM((2,) + block, f32),
            pltpu.VMEM(block, f32),
            pltpu.VMEM((3, 2) + block, bf16),
            pltpu.VMEM((2, count - 1, 2, 128), f32),
            pltpu.VMEM((2, 2, 128), f32),
            pltpu.SemaphoreType.DMA((4,)),
            pltpu.SemaphoreType.DMA((8,)),
            pltpu.SemaphoreType.DMA((12,)),
            pltpu.SemaphoreType.DMA((2,)),
            pltpu.SemaphoreType.DMA((2,)),
        ],
        compiler_params=pltpu.CompilerParams(
            collective_id=0, has_side_effects=True, vmem_limit_bytes=60 * 1024 * 1024
        ),
        name="bond_update",
    )(sector_size, site_tensor, left_env, right_env)
    return pl.pallas_call(
        write_out,
        out_shape=(
            jax.ShapeDtypeStruct(site_tensor.shape, f32),
            jax.ShapeDtypeStruct((1,) + block, f32),
        ),
        in_specs=[inside, inside],
        out_specs=(anywhere, anywhere),
        scratch_shapes=[pltpu.SemaphoreType.DMA((2,))],
        compiler_params=pltpu.CompilerParams(vmem_limit_bytes=4 * 1024 * 1024),
        name="write_out",
    )(left_out, bond_out)


def solution(mesh):
    placed = (
        P(("real", "row"), None, None, None),
        P(("real", "row"), None, None, None),
        P(("real", "row"), None, None, None),
        P("real"),
    )
    return jax.shard_map(
        on_device,
        mesh=mesh,
        in_specs=placed,
        out_specs=(P(("real", "row"), None, None, None), P(("real", "row"), None, None)),
        check_vma=False,
    )
```

```python
import jax
import jax.numpy as jnp
from jax import lax
from jax.experimental import pallas as pl
from jax.experimental.pallas import tpu as pltpu
from jax.sharding import PartitionSpec as P

SIDE = 4
EARLY = 3
QUAD = 4
PANEL = 16
TAU = 0.15
highest = lax.Precision.HIGHEST
f32 = jnp.float32
bf16 = jnp.bfloat16
MESH = pl.DeviceIdType.MESH


def dot(a, b):
    return jnp.dot(a, b, preferred_element_type=f32)


def exact_dot(a, b, dims):
    return lax.dot_general(a, b, (dims, ((), ())), precision=highest, preferred_element_type=f32)


def split_2(value):
    high = value.astype(bf16)
    return high, (value - high.astype(f32)).astype(bf16)


def split_3(value):
    high = value.astype(bf16)
    rest = value - high.astype(f32)
    middle = rest.astype(bf16)
    return high, middle, (rest - middle.astype(f32)).astype(bf16)


def store_split(pair_ref, index, value):
    high, low = split_2(value)
    pair_ref[0, index] = high
    pair_ref[1, index] = low


def row_sum(value):
    rows, columns = value.shape
    summed = jnp.sum(value.reshape(rows // 8, 8, columns), axis=0)
    total = summed[:, :128]
    for start in range(128, columns, 128):
        total = total + summed[:, start : start + 128]
    return jnp.sum(total, axis=0, keepdims=True)


def square(top_left, top_right, bottom_left, bottom_right):
    top = jnp.concatenate([top_left, top_right], 1)
    return jnp.concatenate([top, jnp.concatenate([bottom_left, bottom_right], 1)], 0)


def panel_step(p, lo, hi, states, aug_ref, out_ref):
    base = pl.multiple_of(p * PANEL, PANEL)
    row_id = lax.broadcasted_iota(jnp.int32, (PANEL, 128), 0)
    offset = lax.rem(p * PANEL, 128)
    diag = aug_ref[pl.ds(base, PANEL), lo : lo + 128]
    diag = pltpu.roll(diag, lax.rem(128 - offset, 128), 1)
    columns = [jnp.broadcast_to(diag[:, r : r + 1], (PANEL, 128)) for r in range(PANEL)]
    tiles = [aug_ref[pl.ds(base, PANEL), t : t + 128] for t in range(lo, hi, 128)]
    scale = jnp.zeros((PANEL, 128), f32)
    for r in range(PANEL):
        inverse = lax.rsqrt(columns[r][r : r + 1, :])
        scale = jnp.where(row_id == r, inverse, scale)
        multiplier = columns[r] * inverse
        below = jnp.where(row_id > r, multiplier, 0.0)
        for s in range(r + 1, PANEL):
            columns[s] = columns[s] - below * multiplier[s : s + 1, :]
        if r < PANEL - 1:
            tiles = [tile - below * (tile[r : r + 1, :] * inverse) for tile in tiles]
    tiles = [tile * scale for tile in tiles]
    for t, tile in zip(range(lo, hi, 128), tiles):
        out_ref[pl.ds(base, PANEL), t : t + 128] = tile
    panel = jnp.concatenate(tiles, 1)
    q1, q2, q3 = split_3(panel)
    p1, p2, p3 = (q[:, : states - lo] for q in (q1, q2, q3))
    left = jnp.concatenate([p1, p1, p2, p2, p1, p3], 0)
    right = jnp.concatenate([q1, q2, q1, q2, q3, q1], 0)
    update = lax.dot_general(left, right, (((0,), (0,)), ((), ())), preferred_element_type=f32)
    aug_ref[lo:states, lo:hi] -= update


def kernel(
    size_hbm, site_hbm, left_hbm, right_hbm,
    left_out, bond_out,
    size_ref, site, gram_own, gram_in, left_f, right_f, left_s, right_s, aug, fac, bond_own, bond_in, inv_own, inv_in,
    bond, applied, applied_in, acc, field_s, red_in, red_own, relayed,
    local_sem, send_sem, recv_sem, red_send, red_recv, relay_send, relay_recv, greetings,
):
    count = lax.axis_size("row")
    me = lax.axis_index("row")
    states = site.shape[-1]
    half = states // 2
    channels = left_f.shape[0]
    moved = 2 * SIDE
    not_first, not_last = me > 0, me < count - 1
    to_right, to_left = jnp.minimum(me + 1, count - 1), jnp.maximum(me - 1, 0)

    loads = [
        pltpu.make_async_copy(site_hbm.at[0], site, local_sem.at[0]),
        pltpu.make_async_copy(left_hbm.at[0], left_f, local_sem.at[1]),
        pltpu.make_async_copy(right_hbm.at[0, moved:], right_f.at[moved:], local_sem.at[2]),
    ]
    load_size = pltpu.make_async_copy(size_hbm, size_ref, local_sem.at[3])
    load_size.start()
    for load in loads:
        load.start()

    barrier = pltpu.get_barrier_semaphore()

    def greet(semaphore, distance):
        for there, peer in ((me >= distance, me - distance), (me < count - distance, me + distance)):

            @pl.when(there)
            def _():
                pl.semaphore_signal(semaphore, inc=1, device_id={"row": peer}, device_id_type=MESH)

    def greeted(semaphore, distance):
        peers_of = jnp.where(me >= distance, 1, 0) + jnp.where(me < count - distance, 1, 0)
        pl.semaphore_wait(semaphore, peers_of)

    levels = (count - 1).bit_length()

    def know(level):
        greeted(greetings.at[level], 2**level)
        if level + 1 < levels:
            greet(greetings.at[level + 1], 2 ** (level + 1))

    greet(barrier, 1)

    def remote(source, target, sent, received, peer):
        return pltpu.make_async_remote_copy(
            src_ref=source, dst_ref=target, send_sem=send_sem.at[sent], recv_sem=recv_sem.at[received],
            device_id={"row": peer}, device_id_type=MESH,
        )

    halves = [slice(0, half), slice(half, states)]
    peers = (to_right, to_left)

    def block_copy(side, k, peer):
        a = side * SIDE + k
        return remote(right_hbm.at[0, a], right_f.at[a], 1 + side, (1 if k < EARLY else 3) + side, peer)

    def blocks_sent(side):
        channels_of = pl.ds(side * SIDE, SIDE)
        return remote(right_hbm.at[0, channels_of], right_f.at[channels_of], 1 + side, 1 + side, to_right)

    def early_blocks(side):
        channels_of = pl.ds(side * SIDE, EARLY)
        return remote(right_hbm.at[0, channels_of], right_f.at[channels_of], 1 + side, 1 + side, to_right)

    def bond_copy(side, peer):
        return remote(bond_own, bond_in.at[side], 3 + side, 5 + side, peer)

    def applied_copy(side, part, peer):
        rows = halves[part]
        return remote(applied.at[rows], applied_in.at[side, rows], 5 + side, 7 + 2 * side + part, peer)

    def applied_sent(side):
        return remote(applied, applied_in.at[side], 5 + side, 7 + 2 * side, to_right)

    quads = count // QUAD
    quad, place = me // QUAD, lax.rem(me, QUAD)
    goes_up = quad * SIDE // quads if count % QUAD == 0 else 0 * quad
    goes_down = SIDE - (quad + 1) * SIDE // quads if count % QUAD == 0 else 0 * quad
    relays_up, relays_down = place == QUAD - 1, place == 0
    by_relay = (jnp.where(relays_up, goes_down, 0), jnp.where(relays_down, goes_up, 0))
    relay_amount = jnp.where(relays_up, goes_up, jnp.where(relays_down, goes_down, 0))
    across = jnp.clip(jnp.where(relays_up, me - QUAD + 1, me + QUAD - 1), 0, count - 1)
    beyond = jnp.clip(jnp.where(relays_up, me - QUAD, me + QUAD), 0, count - 1)
    relay_side = jnp.where(relays_up, 1, 0)

    def to_relay(side, k):
        return pltpu.make_async_remote_copy(
            src_ref=right_hbm.at[0, side * SIDE + k], dst_ref=relayed.at[k],
            send_sem=send_sem.at[1 + side], recv_sem=relay_recv.at[k],
            device_id={"row": across}, device_id_type=MESH,
        )

    def from_relay(k):
        return pltpu.make_async_remote_copy(
            src_ref=relayed.at[k], dst_ref=right_f.at[relay_side * SIDE + k],
            send_sem=relay_send.at[k], recv_sem=recv_sem.at[1 + relay_side],
            device_id={"row": beyond}, device_id_type=MESH,
        )

    def start_early(side):
        for k in range(EARLY):

            @pl.when(k < by_relay[side])
            def _():
                to_relay(side, k).start()

            @pl.when(k >= by_relay[side])
            def _():
                sends[side][k].start()

    send_gram = remote(gram_own, gram_in, 0, 0, to_right)
    send_inv = remote(inv_own, inv_in, 7, 11, to_left)
    sends = [[block_copy(s, k, peers[s]) for k in range(SIDE)] for s in range(2)]
    send_bond = [bond_copy(s, peers[s]) for s in range(2)]
    send_applied = [[applied_copy(s, part, peers[s]) for part in range(2)] for s in range(2)]

    load_size.wait()
    size = size_ref[me]
    size_before = size_ref[to_left]
    size_after = size_ref[to_right]
    row = lax.broadcasted_iota(jnp.int32, (states, states), 0)
    column = lax.broadcasted_iota(jnp.int32, (states, states), 1)
    block_row, block_column = row[:half, :half], column[:half, :half]
    on_diagonal = block_row == block_column
    live_pair = (row < size) & (column < size)

    @pl.when(me == 0)
    def _():
        gram_in[...] = jnp.zeros_like(gram_in)
        right_f[:SIDE] = jnp.zeros((SIDE, states, states), f32)
        bond_in[0] = jnp.zeros(bond_in.shape[1:], f32)
        applied_in[0] = jnp.zeros((states, states), f32)

    @pl.when(me == count - 1)
    def _():
        right_f[SIDE:moved] = jnp.zeros((SIDE, states, states), f32)
        bond_in[1] = jnp.zeros(bond_in.shape[1:], f32)
        applied_in[1] = jnp.zeros((states, states), f32)
        inv_in[...] = jnp.zeros_like(inv_in)

    def diagonal_rows(block):
        values = jnp.sum(jnp.where(on_diagonal, block, 0.0), axis=0, keepdims=True)
        return jnp.broadcast_to(values, (8, half))

    def store_packed(packed_ref, block, right_block, diagonal):
        packed_ref[:half, :half] = block
        packed_ref[:half, half:] = right_block
        packed_ref[half:, :half] = diagonal
        packed_ref[half:, half:] = diagonal

    loads[0].wait()
    gram_dims = ((0,), (0,))
    outer = jnp.where((row < size) & (column < size_after), site[1], 0.0)
    gram = exact_dot(outer, outer, gram_dims)
    store_packed(
        gram_own, jnp.where(block_column >= block_row, gram[:half, :half], gram[half:, half:]),
        gram[:half, half:], diagonal_rows(gram[half:, half:]),
    )
    greeted(barrier, 1)
    greet(greetings.at[0], 1)

    @pl.when(not_last)
    def _():
        send_gram.start()

    upper = jnp.where(live_pair, site[0], 0.0)
    site[0] = upper
    gram = exact_dot(upper, upper, gram_dims)
    gram = gram + jnp.where((row == column) & (row >= size), 1.0, 0.0)
    aug[:, states:] = jnp.where(row == column, 1.0, 0.0).astype(f32)
    fac[...] = jnp.zeros_like(fac)
    know(0)

    @pl.when(not_last)
    def _():
        send_gram.wait_send()

    know(1)

    waits_down, waits_up = not_last & (place == 1), not_first & (place == 2)

    @pl.when(not_last & ~waits_down)
    def _():
        start_early(0)


    @pl.when(not_first)
    def _():
        send_gram.wait_recv()

    @pl.when(not_first & ~waits_up)
    def _():
        start_early(1)

    block = gram_in[:half, :half]
    mirrored = block.T
    top_left = jnp.where(block_column >= block_row, block, mirrored)
    bottom_right = jnp.where(block_column < block_row, block, jnp.where(on_diagonal, gram_in[half : half + 1, :half], mirrored))
    aug[:half, :half] = gram[:half, :half] + top_left
    aug[:half, half:states] = gram[:half, half:] + gram_in[:half, half:]
    aug[half:, :half] = gram[half:, :half]
    aug[half:, half:states] = gram[half:, half:] + bottom_right
    loads[1].wait()
    loads[2].wait()

    panels = half // PANEL

    def first_half(p, carry):
        panel_step(p, 0, states + half, states, aug, fac)
        store_split(left_s, p, left_f[p])
        return carry

    def second_half(p, carry):
        panel_step(p, half, 2 * states, states, aug, fac)
        other = jnp.minimum(p, channels - 1)
        store_split(left_s, other, left_f[other])
        mine = jnp.minimum(p - panels + moved, channels - 1)
        store_split(right_s, mine, right_f[mine])
        return carry

    lax.fori_loop(0, panels, first_half, 0)
    know(2)

    @pl.when(waits_down)
    def _():
        start_early(0)

    @pl.when(waits_up)
    def _():
        start_early(1)

    lax.fori_loop(panels, 2 * panels, second_half, 0)
    for level in range(3, levels):
        know(level)

    bottom_right = fac[half:, half:states]
    store_packed(
        bond_own, jnp.where(block_column >= block_row, fac[:half, :half], bottom_right.T),
        fac[:half, half:states], diagonal_rows(bottom_right),
    )

    @pl.when(not_last)
    def _():
        for one in [send_bond[0]] + sends[0][EARLY:]:
            one.start()

    @pl.when(not_first)
    def _():
        for one in [send_bond[1]] + sends[1][EARLY:]:
            one.start()

    bond[...] = jnp.where(live_pair & (column >= row), fac[:, :states], 0.0)

    def relay(start, stop):
        for k in range(start, stop):

            @pl.when(k < relay_amount)
            def _():
                to_relay(0, k).wait_recv()
                from_relay(k).start()

    relay(0, 2)

    def put_field(which, value):
        field_s[which, 0], field_s[which, 1] = split_2(value)

    def middle_of(which, a, rows):
        high, low_part = field_s[which, 0, rows], field_s[which, 1, rows]
        r_high, r_low = right_s[0, a], right_s[1, a]
        return split_2(dot(high, r_high) + dot(high, r_low) + dot(low_part, r_high))

    def outside(total, l_high, l_low, m_high, m_low):
        return total + dot(l_high, m_high) + dot(l_high, m_low) + dot(l_low, m_high)

    def add_terms(total, which, a):
        m_high, m_low = middle_of(which, a, slice(None))
        return outside(total, left_s[0, a], left_s[1, a], m_high, m_low)

    def add_range(which, start, amount):
        group = next(n for n in (3, 2, 1) if amount % n == 0)

        def some(g, carry):
            total = acc[...]
            for k in range(group):
                total = add_terms(total, which, start + g * group + k)
            acc[...] = total
            return carry

        lax.fori_loop(0, amount // group, some, 0)

    near = 1 - lax.rem(me, 2)
    has_side = [jnp.where(s == 0, not_first, not_last) for s in (near, 1 - near)]
    sides = list(zip((near, 1 - near), has_side))

    acc[...] = jnp.zeros_like(acc)
    put_field(0, bond[...])
    add_range(0, moved, channels - moved)
    relay(2, EARLY)
    inverse = jnp.where(column <= row, fac[:, states:], 0.0)
    turned = ((1,), (1,))
    left_out[0] = exact_dot(site[0], inverse, turned)
    inv_own[:, :half] = jnp.where(block_column < block_row, inverse[:half, :half], inverse[half:, half:].T)
    inv_own[:, half:] = inverse[half:, :half]

    for order, (side, there) in enumerate(sides):

        @pl.when(there)
        def _():
            bond_copy(side, to_right).wait_recv()

        limit = jnp.where(side == 0, size_before, size_after)
        block = bond_in[side, :half, :half]
        top_left = jnp.where(block_column >= block_row, block, 0.0)
        bottom_right = jnp.where(block_column > block_row, block.T, jnp.where(on_diagonal, bond_in[side, half : half + 1, :half], 0.0))
        field = square(top_left, bond_in[side, :half, half:], jnp.zeros((half, half), f32), bottom_right)
        put_field(1 + side, jnp.where((row < limit) & (column < limit), field, 0.0))

        @pl.when(there)
        def _():
            early_blocks(side).wait_recv()

        for k in range(EARLY):
            store_split(right_s, side * SIDE + k, right_f[side * SIDE + k])
        total = acc[...]
        for k in range(EARLY):
            total = add_terms(total, 1 + side, side * SIDE + k)
        acc[...] = total

        @pl.when(there)
        def _():
            block_copy(side, EARLY, to_right).wait_recv()

        last = side * SIDE + EARLY
        store_split(right_s, last, right_f[last])
        if order == 0:
            acc[...] = add_terms(acc[...], 1 + side, last)

    def reductions(t):
        for step in range(1, count):
            peer = lax.rem(me + step, count)
            yield pltpu.make_async_remote_copy(
                src_ref=red_own.at[t], dst_ref=red_in.at[t, step - 1],
                send_sem=red_send.at[t], recv_sem=red_recv.at[t],
                device_id={"row": peer}, device_id_type=MESH,
            )

    def all_reductions(t):
        return pltpu.make_async_remote_copy(
            src_ref=red_in.at[t], dst_ref=red_in.at[t], send_sem=red_send.at[t], recv_sem=red_recv.at[t],
            device_id={"row": to_right}, device_id_type=MESH,
        )

    held = (not_last & (place == QUAD - 1), not_first & (place == 0))
    last = (1 - near) * SIDE + EARLY
    m_high, m_low = middle_of(2 - near, last, slice(None))
    for part, rows in enumerate(halves):
        value = outside(acc[rows], left_s[0, last, rows], left_s[1, last, rows], m_high, m_low)
        applied[rows] = jnp.where(live_pair[rows], value, 0.0)
        if part == 1:
            red_own[0, :1] = row_sum(bond[...] * bond[...])
            red_own[0, 1:] = row_sum(bond[...] * applied[...])
            for one in reductions(0):
                one.start()

        @pl.when(not_last & ~held[0])
        def _():
            send_applied[0][part].start()

        @pl.when(not_first & ~held[1])
        def _():
            send_applied[1][part].start()

    acc[...] = jnp.zeros_like(acc)
    put_field(0, applied[...])
    first_own = (channels - moved) // 2
    add_range(0, moved, first_own)
    add_range(0, moved + first_own, channels - moved - first_own)

    for order, (side, there) in enumerate(sides):
        for part, rows in enumerate(halves):

            @pl.when(there)
            def _():
                applied_copy(side, part, to_right).wait_recv()

            if order == 0 and part == 0:
                for s in range(2):

                    @pl.when(held[s])
                    def _():
                        for one in send_applied[s]:
                            one.start()

            if order == 1 and part == 1:

                @pl.when(not_first)
                def _():
                    send_inv.start()

            which = 1 + side
            field_s[which, 0, rows], field_s[which, 1, rows] = split_2(applied_in[side, rows])
            middles = [middle_of(which, side * SIDE + k, rows) for k in range(SIDE)]
            total = acc[...]
            for k in range(0, SIDE, 2):
                pair = [side * SIDE + k, side * SIDE + k + 1]
                l_high, l_low = (jnp.concatenate([left_s[i, a, :, rows] for a in pair], 1) for i in range(2))
                m_high, m_low = (jnp.concatenate([middles[k + j][i] for j in range(2)], 0) for i in range(2))
                total = outside(total, l_high, l_low, m_high, m_low)
            acc[...] = total

    def collect(t):
        all_reductions(t).wait_recv()
        return jnp.sum(red_own[t] + jnp.sum(red_in[t], axis=0), axis=1, keepdims=True)

    total = collect(0)
    start_norm = total[:1]
    energy = total[1:] / start_norm
    shifted = applied[...] - energy * bond[...]
    second = jnp.where(live_pair, acc[...], 0.0) - energy * applied[...] - energy * shifted
    acc[...] = bond[...] + TAU * shifted + (0.5 * TAU * TAU) * second
    red_own[1, :1] = row_sum(acc[...] * acc[...])
    red_own[1, 1:] = jnp.zeros((1, 128), f32)
    for one in reductions(1):
        one.start()


    @pl.when(not_last)
    def _():
        send_inv.wait_recv()

    block = inv_in[:, :half]
    near_block, near_low = bond_in[1, :half, :half], bond_in[1, half : half + 1, :half]
    zeros = jnp.zeros((half, half), f32)
    top_left = jnp.where(block_column < block_row, block, jnp.where(on_diagonal, 1.0 / near_block, 0.0))
    bottom_right = jnp.where(block_column < block_row, block.T, jnp.where(on_diagonal, 1.0 / near_low, 0.0))
    outer = jnp.where((row < size) & (column < size_after), site[1], 0.0)
    outer = exact_dot(outer, square(top_left, zeros, inv_in[:, half:], bottom_right), turned)
    left_out[1] = jnp.where(not_last, outer, 0.0)

    @pl.when(not_last)
    def _():
        for one in [blocks_sent(0), send_bond[0], applied_sent(0)]:
            one.wait_send()

    @pl.when(not_first)
    def _():
        for one in [blocks_sent(1), send_bond[1], applied_sent(1), send_inv]:
            one.wait_send()

    for k in range(EARLY):

        @pl.when(k < relay_amount)
        def _():
            from_relay(k).wait_send()

    final_norm = collect(1)[:1]
    bond_out[...] = acc[...] * jnp.sqrt(start_norm / final_norm)
    for t in range(2):
        all_reductions(t).wait_send()


def write_out(left, bond, left_hbm, bond_hbm, sem):
    stores = [
        pltpu.make_async_copy(left, left_hbm.at[0], sem.at[0]),
        pltpu.make_async_copy(bond, bond_hbm.at[0], sem.at[1]),
    ]
    for store in stores:
        store.start()
    for store in stores:
        store.wait()


def on_device(site_tensor, left_env, right_env, sector_size):
    states = site_tensor.shape[-1]
    channels = left_env.shape[1]
    count = lax.axis_size("row")
    block = (states, states)
    triangle = (states // 2 + 8, states)
    anywhere = pl.BlockSpec(memory_space=pl.ANY)
    inside = pl.BlockSpec(memory_space=pltpu.VMEM)
    left_out, bond_out = pl.pallas_call(
        kernel,
        out_shape=(
            pltpu.VMEM((2,) + block, f32),
            pltpu.VMEM(block, f32),
        ),
        in_specs=[pl.BlockSpec(memory_space=pltpu.HBM)] * 4,
        out_specs=(inside, inside),
        scratch_shapes=[
            pltpu.SMEM(sector_size.shape, jnp.int32),
            pltpu.VMEM((2,) + block, f32),
            pltpu.VMEM(triangle, f32),
            pltpu.VMEM(triangle, f32),
            pltpu.VMEM((channels,) + block, f32),
            pltpu.VMEM((channels,) + block, f32),
            pltpu.VMEM((2, channels) + block, bf16),
            pltpu.VMEM((2, channels) + block, bf16),
            pltpu.VMEM((states, 2 * states), f32),
            pltpu.VMEM((states, 2 * states), f32),
            pltpu.VMEM(triangle, f32),
            pltpu.VMEM((2,) + triangle, f32),
            pltpu.VMEM((states // 2, states), f32),
            pltpu.VMEM((states // 2, states), f32),
            pltpu.VMEM(block, f32),
            pltpu.VMEM(block, f32),
            pltpu.VMEM((2,) + block, f32),
            pltpu.VMEM(block, f32),
            pltpu.VMEM((3, 2) + block, bf16),
            pltpu.VMEM((2, count - 1, 2, 128), f32),
            pltpu.VMEM((2, 2, 128), f32),
            pltpu.VMEM((EARLY,) + block, f32),
            pltpu.SemaphoreType.DMA((4,)),
            pltpu.SemaphoreType.DMA((8,)),
            pltpu.SemaphoreType.DMA((12,)),
            pltpu.SemaphoreType.DMA((2,)),
            pltpu.SemaphoreType.DMA((2,)),
            pltpu.SemaphoreType.DMA((EARLY,)),
            pltpu.SemaphoreType.DMA((EARLY,)),
            pltpu.SemaphoreType.REGULAR(((count - 1).bit_length(),)),
        ],
        compiler_params=pltpu.CompilerParams(
            collective_id=0, has_side_effects=True, vmem_limit_bytes=60 * 1024 * 1024
        ),
        name="bond_update",
    )(sector_size, site_tensor, left_env, right_env)
    return pl.pallas_call(
        write_out,
        out_shape=(
            jax.ShapeDtypeStruct(site_tensor.shape, f32),
            jax.ShapeDtypeStruct((1,) + block, f32),
        ),
        in_specs=[inside, inside],
        out_specs=(anywhere, anywhere),
        scratch_shapes=[pltpu.SemaphoreType.DMA((2,))],
        compiler_params=pltpu.CompilerParams(vmem_limit_bytes=4 * 1024 * 1024),
        name="write_out",
    )(left_out, bond_out)


def solution(mesh):
    placed = (
        P(("real", "row"), None, None, None),
        P(("real", "row"), None, None, None),
        P(("real", "row"), None, None, None),
        P("real"),
    )
    return jax.shard_map(
        on_device,
        mesh=mesh,
        in_specs=placed,
        out_specs=(P(("real", "row"), None, None, None), P(("real", "row"), None, None)),
        check_vma=False,
    )
```

```python
import jax
import jax.numpy as jnp
from jax import lax
from jax.experimental import pallas as pl
from jax.experimental.pallas import tpu as pltpu
from jax.sharding import PartitionSpec as P

SIDE = 4
EARLY = 3
QUAD = 4
PANEL = 16
TAU = 0.15
highest = lax.Precision.HIGHEST
f32 = jnp.float32
bf16 = jnp.bfloat16
MESH = pl.DeviceIdType.MESH


def dot(a, b):
    return jnp.dot(a, b, preferred_element_type=f32)


def exact_dot(a, b, dims):
    return lax.dot_general(a, b, (dims, ((), ())), precision=highest, preferred_element_type=f32)


def split_2(value):
    high = value.astype(bf16)
    return high, (value - high.astype(f32)).astype(bf16)


def split_3(value):
    high = value.astype(bf16)
    rest = value - high.astype(f32)
    middle = rest.astype(bf16)
    return high, middle, (rest - middle.astype(f32)).astype(bf16)


def store_split(pair_ref, index, value):
    high, low = split_2(value)
    pair_ref[0, index] = high
    pair_ref[1, index] = low


def row_sum(value):
    rows, columns = value.shape
    summed = jnp.sum(value.reshape(rows // 8, 8, columns), axis=0)
    total = summed[:, :128]
    for start in range(128, columns, 128):
        total = total + summed[:, start : start + 128]
    return jnp.sum(total, axis=0, keepdims=True)


def square(top_left, top_right, bottom_left, bottom_right):
    top = jnp.concatenate([top_left, top_right], 1)
    return jnp.concatenate([top, jnp.concatenate([bottom_left, bottom_right], 1)], 0)


def panel_step(p, lo, hi, states, aug_ref, out_ref):
    base = pl.multiple_of(p * PANEL, PANEL)
    row_id = lax.broadcasted_iota(jnp.int32, (PANEL, 128), 0)
    offset = lax.rem(p * PANEL, 128)
    diag = aug_ref[pl.ds(base, PANEL), lo : lo + 128]
    diag = pltpu.roll(diag, lax.rem(128 - offset, 128), 1)
    columns = [jnp.broadcast_to(diag[:, r : r + 1], (PANEL, 128)) for r in range(PANEL)]
    tiles = [aug_ref[pl.ds(base, PANEL), t : t + 128] for t in range(lo, hi, 128)]
    scale = jnp.zeros((PANEL, 128), f32)
    for r in range(PANEL):
        inverse = lax.rsqrt(columns[r][r : r + 1, :])
        scale = jnp.where(row_id == r, inverse, scale)
        multiplier = columns[r] * inverse
        below = jnp.where(row_id > r, multiplier, 0.0)
        for s in range(r + 1, PANEL):
            columns[s] = columns[s] - below * multiplier[s : s + 1, :]
        if r < PANEL - 1:
            tiles = [tile - below * (tile[r : r + 1, :] * inverse) for tile in tiles]
    tiles = [tile * scale for tile in tiles]
    for t, tile in zip(range(lo, hi, 128), tiles):
        out_ref[pl.ds(base, PANEL), t : t + 128] = tile
    panel = jnp.concatenate(tiles, 1)
    q1, q2, q3 = split_3(panel)
    p1, p2, p3 = (q[:, : states - lo] for q in (q1, q2, q3))
    left = jnp.concatenate([p1, p1, p2, p2, p1, p3], 0)
    right = jnp.concatenate([q1, q2, q1, q2, q3, q1], 0)
    update = lax.dot_general(left, right, (((0,), (0,)), ((), ())), preferred_element_type=f32)
    aug_ref[lo:states, lo:hi] -= update


def kernel(
    size_hbm, site_hbm, left_hbm, right_hbm,
    left_out, bond_out,
    size_ref, site, gram_own, gram_in, left_f, right_f, left_s, right_s, aug, fac, bond_own, bond_in, inv_own, inv_in,
    bond, applied, applied_in, acc, field_s, red_in, red_own, relayed,
    local_sem, send_sem, recv_sem, red_send, red_recv, relay_send, relay_recv, greetings, go,
):
    count = lax.axis_size("row")
    me = lax.axis_index("row")
    states = site.shape[-1]
    half = states // 2
    channels = left_f.shape[0]
    moved = 2 * SIDE
    not_first, not_last = me > 0, me < count - 1
    to_right, to_left = jnp.minimum(me + 1, count - 1), jnp.maximum(me - 1, 0)

    loads = [
        pltpu.make_async_copy(site_hbm.at[0], site, local_sem.at[0]),
        pltpu.make_async_copy(left_hbm.at[0], left_f, local_sem.at[1]),
        pltpu.make_async_copy(right_hbm.at[0, moved:], right_f.at[moved:], local_sem.at[2]),
    ]
    load_size = pltpu.make_async_copy(size_hbm, size_ref, local_sem.at[3])
    load_size.start()
    for load in loads:
        load.start()

    quads = count // QUAD
    quad, place = me // QUAD, lax.rem(me, QUAD)
    goes_up = quad * SIDE // quads if count % QUAD == 0 else 0 * quad
    goes_down = SIDE - (quad + 1) * SIDE // quads if count % QUAD == 0 else 0 * quad
    relays_up, relays_down = place == QUAD - 1, place == 0
    paired = relays_up | relays_down if count % QUAD == 0 else me < 0
    across = jnp.clip(jnp.where(relays_up, me - QUAD + 1, me + QUAD - 1), 0, count - 1)
    frees = ((place == 1) & (me + QUAD - 1 < count), (place == 2) & (me >= QUAD - 1))
    over = (jnp.minimum(me + QUAD - 1, count - 1), jnp.maximum(me - QUAD + 1, 0))

    barrier = pltpu.get_barrier_semaphore()

    def greet(semaphore, distance):
        for there, peer in ((me >= distance, me - distance), (me < count - distance, me + distance)):

            @pl.when(there)
            def _():
                pl.semaphore_signal(semaphore, inc=1, device_id={"row": peer}, device_id_type=MESH)

    def greeted(semaphore, distance, more=0):
        peers_of = jnp.where(me >= distance, 1, 0) + jnp.where(me < count - distance, 1, 0)
        pl.semaphore_wait(semaphore, peers_of + more)

    levels = (count - 1).bit_length()

    def know(level):
        greeted(greetings.at[level], 2**level)
        if level + 1 < levels:
            greet(greetings.at[level + 1], 2 ** (level + 1))

    greet(barrier, 1)

    @pl.when(paired)
    def _():
        pl.semaphore_signal(barrier, inc=1, device_id={"row": across}, device_id_type=MESH)


    def remote(source, target, sent, received, peer):
        return pltpu.make_async_remote_copy(
            src_ref=source, dst_ref=target, send_sem=send_sem.at[sent], recv_sem=recv_sem.at[received],
            device_id={"row": peer}, device_id_type=MESH,
        )

    halves = [slice(0, half), slice(half, states)]
    peers = (to_right, to_left)

    def block_copy(side, k, peer):
        a = side * SIDE + k
        return remote(right_hbm.at[0, a], right_f.at[a], 1 + side, (1 if k < EARLY else 3) + side, peer)

    def blocks_sent(side):
        channels_of = pl.ds(side * SIDE, SIDE)
        return remote(right_hbm.at[0, channels_of], right_f.at[channels_of], 1 + side, 1 + side, to_right)

    def early_blocks(side):
        channels_of = pl.ds(side * SIDE, EARLY)
        return remote(right_hbm.at[0, channels_of], right_f.at[channels_of], 1 + side, 1 + side, to_right)

    def bond_copy(side, peer):
        return remote(bond_own, bond_in.at[side], 3 + side, 5 + side, peer)

    def applied_copy(side, part, peer):
        rows = halves[part]
        return remote(applied.at[rows], applied_in.at[side, rows], 5 + side, 7 + 2 * side + part, peer)

    def applied_sent(side):
        return remote(applied, applied_in.at[side], 5 + side, 7 + 2 * side, to_right)

    by_relay = (jnp.where(relays_up, goes_down, 0), jnp.where(relays_down, goes_up, 0))
    relay_amount = jnp.where(relays_up, goes_up, jnp.where(relays_down, goes_down, 0))
    beyond = jnp.clip(jnp.where(relays_up, me - QUAD, me + QUAD), 0, count - 1)
    relay_side = jnp.where(relays_up, 1, 0)

    def to_relay(side, k):
        return pltpu.make_async_remote_copy(
            src_ref=right_hbm.at[0, side * SIDE + k], dst_ref=relayed.at[k],
            send_sem=send_sem.at[1 + side], recv_sem=relay_recv.at[k],
            device_id={"row": across}, device_id_type=MESH,
        )

    def from_relay(k):
        return pltpu.make_async_remote_copy(
            src_ref=relayed.at[k], dst_ref=right_f.at[relay_side * SIDE + k],
            send_sem=relay_send.at[k], recv_sem=recv_sem.at[1 + relay_side],
            device_id={"row": beyond}, device_id_type=MESH,
        )

    def start_relayed(side):
        for k in range(EARLY):

            @pl.when(k < by_relay[side])
            def _():
                to_relay(side, k).start()

    def start_early(side):
        for k in range(EARLY):

            @pl.when(k >= by_relay[side])
            def _():
                sends[side][k].start()

    send_gram = remote(gram_own, gram_in, 0, 0, to_right)
    send_inv = remote(inv_own, inv_in, 7, 11, to_left)
    sends = [[block_copy(s, k, peers[s]) for k in range(SIDE)] for s in range(2)]
    send_bond = [bond_copy(s, peers[s]) for s in range(2)]
    send_applied = [[applied_copy(s, part, peers[s]) for part in range(2)] for s in range(2)]

    load_size.wait()
    size = size_ref[me]
    size_before = size_ref[to_left]
    size_after = size_ref[to_right]
    row = lax.broadcasted_iota(jnp.int32, (states, states), 0)
    column = lax.broadcasted_iota(jnp.int32, (states, states), 1)
    block_row, block_column = row[:half, :half], column[:half, :half]
    on_diagonal = block_row == block_column
    live_pair = (row < size) & (column < size)

    @pl.when(me == 0)
    def _():
        gram_in[...] = jnp.zeros_like(gram_in)
        right_f[:SIDE] = jnp.zeros((SIDE, states, states), f32)
        bond_in[0] = jnp.zeros(bond_in.shape[1:], f32)
        applied_in[0] = jnp.zeros((states, states), f32)

    @pl.when(me == count - 1)
    def _():
        right_f[SIDE:moved] = jnp.zeros((SIDE, states, states), f32)
        bond_in[1] = jnp.zeros(bond_in.shape[1:], f32)
        applied_in[1] = jnp.zeros((states, states), f32)
        inv_in[...] = jnp.zeros_like(inv_in)

    def diagonal_rows(block):
        values = jnp.sum(jnp.where(on_diagonal, block, 0.0), axis=0, keepdims=True)
        return jnp.broadcast_to(values, (8, half))

    def store_packed(packed_ref, block, right_block, diagonal):
        packed_ref[:half, :half] = block
        packed_ref[:half, half:] = right_block
        packed_ref[half:, :half] = diagonal
        packed_ref[half:, half:] = diagonal

    loads[0].wait()
    gram_dims = ((0,), (0,))
    outer = jnp.where((row < size) & (column < size_after), site[1], 0.0)
    gram = exact_dot(outer, outer, gram_dims)
    store_packed(
        gram_own, jnp.where(block_column >= block_row, gram[:half, :half], gram[half:, half:]),
        gram[:half, half:], diagonal_rows(gram[half:, half:]),
    )
    greeted(barrier, 1, jnp.where(paired, 1, 0))
    greet(greetings.at[0], 1)
    start_relayed(0)

    waits_down, waits_up = not_last & (place == 1), not_first & (place == 2)

    @pl.when(not_last)
    def _():
        send_gram.start()

    @pl.when(not_last & ~waits_down)
    def _():
        start_early(0)

    upper = jnp.where(live_pair, site[0], 0.0)
    site[0] = upper
    gram = exact_dot(upper, upper, gram_dims)
    gram = gram + jnp.where((row == column) & (row >= size), 1.0, 0.0)
    aug[:, states:] = jnp.where(row == column, 1.0, 0.0).astype(f32)
    fac[...] = jnp.zeros_like(fac)
    start_relayed(1)

    @pl.when(not_first & ~waits_up)
    def _():
        start_early(1)

    know(0)

    @pl.when(not_first)
    def _():
        send_gram.wait_recv()

    know(1)
    block = gram_in[:half, :half]
    mirrored = block.T
    top_left = jnp.where(block_column >= block_row, block, mirrored)
    bottom_right = jnp.where(block_column < block_row, block, jnp.where(on_diagonal, gram_in[half : half + 1, :half], mirrored))
    aug[:half, :half] = gram[:half, :half] + top_left
    aug[:half, half:states] = gram[:half, half:] + gram_in[:half, half:]
    aug[half:, :half] = gram[half:, :half]
    aug[half:, half:states] = gram[half:, half:] + bottom_right
    loads[1].wait()
    loads[2].wait()

    panels = half // PANEL

    def first_half(p, carry):
        panel_step(p, 0, states + half, states, aug, fac)
        store_split(left_s, p, left_f[p])
        return carry

    def second_half(p, carry):
        panel_step(p, half, 2 * states, states, aug, fac)
        other = jnp.minimum(p, channels - 1)
        store_split(left_s, other, left_f[other])
        mine = jnp.minimum(p - panels + moved, channels - 1)
        store_split(right_s, mine, right_f[mine])
        return carry

    lax.fori_loop(0, panels // 2, first_half, 0)

    @pl.when(waits_down)
    def _():
        start_early(0)

    @pl.when(waits_up)
    def _():
        start_early(1)

    lax.fori_loop(panels // 2, panels, first_half, 0)
    know(2)
    lax.fori_loop(panels, 2 * panels, second_half, 0)
    for level in range(3, levels):
        know(level)

    bottom_right = fac[half:, half:states]
    store_packed(
        bond_own, jnp.where(block_column >= block_row, fac[:half, :half], bottom_right.T),
        fac[:half, half:states], diagonal_rows(bottom_right),
    )

    @pl.when(not_last)
    def _():
        for one in [send_bond[0]] + sends[0][EARLY:]:
            one.start()

    @pl.when(not_first)
    def _():
        for one in [send_bond[1]] + sends[1][EARLY:]:
            one.start()

    bond[...] = jnp.where(live_pair & (column >= row), fac[:, :states], 0.0)

    def relay(start, stop):
        for k in range(start, stop):

            @pl.when(k < relay_amount)
            def _():
                to_relay(0, k).wait_recv()
                from_relay(k).start()

    relay(0, 2)

    def put_field(which, value):
        field_s[which, 0], field_s[which, 1] = split_2(value)

    def middle_of(which, a, rows):
        high, low_part = field_s[which, 0, rows], field_s[which, 1, rows]
        r_high, r_low = right_s[0, a], right_s[1, a]
        return split_2(dot(high, r_high) + dot(high, r_low) + dot(low_part, r_high))

    def outside(total, l_high, l_low, m_high, m_low):
        return total + dot(l_high, m_high) + dot(l_high, m_low) + dot(l_low, m_high)

    def add_terms(total, which, a):
        m_high, m_low = middle_of(which, a, slice(None))
        return outside(total, left_s[0, a], left_s[1, a], m_high, m_low)

    def add_range(which, start, amount):
        group = next(n for n in (3, 2, 1) if amount % n == 0)

        def some(g, carry):
            total = acc[...]
            for k in range(group):
                total = add_terms(total, which, start + g * group + k)
            acc[...] = total
            return carry

        lax.fori_loop(0, amount // group, some, 0)

    near = 1 - lax.rem(me, 2)
    has_side = [jnp.where(s == 0, not_first, not_last) for s in (near, 1 - near)]
    sides = list(zip((near, 1 - near), has_side))

    acc[...] = jnp.zeros_like(acc)
    put_field(0, bond[...])
    add_range(0, moved, channels - moved)
    relay(2, EARLY)
    inverse = jnp.where(column <= row, fac[:, states:], 0.0)
    turned = ((1,), (1,))
    left_out[0] = exact_dot(site[0], inverse, turned)
    inv_own[:, :half] = jnp.where(block_column < block_row, inverse[:half, :half], inverse[half:, half:].T)
    inv_own[:, half:] = inverse[half:, :half]

    for order, (side, there) in enumerate(sides):

        @pl.when(there)
        def _():
            bond_copy(side, to_right).wait_recv()

        limit = jnp.where(side == 0, size_before, size_after)
        block = bond_in[side, :half, :half]
        top_left = jnp.where(block_column >= block_row, block, 0.0)
        bottom_right = jnp.where(block_column > block_row, block.T, jnp.where(on_diagonal, bond_in[side, half : half + 1, :half], 0.0))
        field = square(top_left, bond_in[side, :half, half:], jnp.zeros((half, half), f32), bottom_right)
        put_field(1 + side, jnp.where((row < limit) & (column < limit), field, 0.0))

        @pl.when(there)
        def _():
            early_blocks(side).wait_recv()

        for k in range(EARLY):
            store_split(right_s, side * SIDE + k, right_f[side * SIDE + k])
        total = acc[...]
        for k in range(EARLY):
            total = add_terms(total, 1 + side, side * SIDE + k)
        acc[...] = total
        if order == 1:
            for s in range(2):

                @pl.when(frees[s])
                def _():
                    blocks_sent(s).wait_send()
                    pl.semaphore_signal(go, inc=1, device_id={"row": over[s]}, device_id_type=MESH)


        @pl.when(there)
        def _():
            block_copy(side, EARLY, to_right).wait_recv()

        last = side * SIDE + EARLY
        store_split(right_s, last, right_f[last])
        if order == 0:
            acc[...] = add_terms(acc[...], 1 + side, last)

    def reductions(t):
        for step in range(1, count):
            peer = lax.rem(me + step, count)
            yield pltpu.make_async_remote_copy(
                src_ref=red_own.at[t], dst_ref=red_in.at[t, step - 1],
                send_sem=red_send.at[t], recv_sem=red_recv.at[t],
                device_id={"row": peer}, device_id_type=MESH,
            )

    def all_reductions(t):
        return pltpu.make_async_remote_copy(
            src_ref=red_in.at[t], dst_ref=red_in.at[t], send_sem=red_send.at[t], recv_sem=red_recv.at[t],
            device_id={"row": to_right}, device_id_type=MESH,
        )

    held = (not_last & (place == QUAD - 1), not_first & (place == 0))
    last = (1 - near) * SIDE + EARLY
    m_high, m_low = middle_of(2 - near, last, slice(None))
    for part, rows in enumerate(halves):
        value = outside(acc[rows], left_s[0, last, rows], left_s[1, last, rows], m_high, m_low)
        applied[rows] = jnp.where(live_pair[rows], value, 0.0)
        if part == 1:
            red_own[0, :1] = row_sum(bond[...] * bond[...])
            red_own[0, 1:] = row_sum(bond[...] * applied[...])
            for one in reductions(0):
                one.start()

        @pl.when(not_last & ~held[0])
        def _():
            send_applied[0][part].start()

        @pl.when(not_first & ~held[1])
        def _():
            send_applied[1][part].start()

    acc[...] = jnp.zeros_like(acc)
    put_field(0, applied[...])
    first_own = (channels - moved) // 2
    add_range(0, moved, first_own)
    add_range(0, moved + first_own, channels - moved - first_own)
    for s in range(2):

        @pl.when(held[s])
        def _():
            pl.semaphore_wait(go, 1)
            for one in send_applied[s]:
                one.start()


    for order, (side, there) in enumerate(sides):
        for part, rows in enumerate(halves):

            @pl.when(there)
            def _():
                applied_copy(side, part, to_right).wait_recv()

            if order == 1 and part == 1:

                @pl.when(not_first)
                def _():
                    send_inv.start()

            which = 1 + side
            field_s[which, 0, rows], field_s[which, 1, rows] = split_2(applied_in[side, rows])
            middles = [middle_of(which, side * SIDE + k, rows) for k in range(SIDE)]
            total = acc[...]
            for k in range(0, SIDE, 2):
                pair = [side * SIDE + k, side * SIDE + k + 1]
                l_high, l_low = (jnp.concatenate([left_s[i, a, :, rows] for a in pair], 1) for i in range(2))
                m_high, m_low = (jnp.concatenate([middles[k + j][i] for j in range(2)], 0) for i in range(2))
                total = outside(total, l_high, l_low, m_high, m_low)
            acc[...] = total

    def collect(t):
        all_reductions(t).wait_recv()
        return jnp.sum(red_own[t] + jnp.sum(red_in[t], axis=0), axis=1, keepdims=True)

    total = collect(0)
    start_norm = total[:1]
    energy = total[1:] / start_norm
    shifted = applied[...] - energy * bond[...]
    second = jnp.where(live_pair, acc[...], 0.0) - energy * applied[...] - energy * shifted
    acc[...] = bond[...] + TAU * shifted + (0.5 * TAU * TAU) * second
    red_own[1, :1] = row_sum(acc[...] * acc[...])
    red_own[1, 1:] = jnp.zeros((1, 128), f32)
    for one in reductions(1):
        one.start()


    @pl.when(not_last)
    def _():
        send_inv.wait_recv()

    block = inv_in[:, :half]
    near_block, near_low = bond_in[1, :half, :half], bond_in[1, half : half + 1, :half]
    zeros = jnp.zeros((half, half), f32)
    top_left = jnp.where(block_column < block_row, block, jnp.where(on_diagonal, 1.0 / near_block, 0.0))
    bottom_right = jnp.where(block_column < block_row, block.T, jnp.where(on_diagonal, 1.0 / near_low, 0.0))
    outer = jnp.where((row < size) & (column < size_after), site[1], 0.0)
    outer = exact_dot(outer, square(top_left, zeros, inv_in[:, half:], bottom_right), turned)
    left_out[1] = jnp.where(not_last, outer, 0.0)

    @pl.when(not_last)
    def _():
        for one in [send_gram, send_bond[0], applied_sent(0)]:
            one.wait_send()

    @pl.when(not_first)
    def _():
        for one in [send_bond[1], applied_sent(1), send_inv]:
            one.wait_send()

    for s, there in enumerate((not_last, not_first)):

        @pl.when(there & ~frees[s])
        def _():
            blocks_sent(s).wait_send()

    for k in range(EARLY):

        @pl.when(k < relay_amount)
        def _():
            from_relay(k).wait_send()

    final_norm = collect(1)[:1]
    bond_out[...] = acc[...] * jnp.sqrt(start_norm / final_norm)
    for t in range(2):
        all_reductions(t).wait_send()


def write_out(left, bond, left_hbm, bond_hbm, sem):
    stores = [
        pltpu.make_async_copy(left, left_hbm.at[0], sem.at[0]),
        pltpu.make_async_copy(bond, bond_hbm.at[0], sem.at[1]),
    ]
    for store in stores:
        store.start()
    for store in stores:
        store.wait()


def on_device(site_tensor, left_env, right_env, sector_size):
    states = site_tensor.shape[-1]
    channels = left_env.shape[1]
    count = lax.axis_size("row")
    block = (states, states)
    triangle = (states // 2 + 8, states)
    anywhere = pl.BlockSpec(memory_space=pl.ANY)
    inside = pl.BlockSpec(memory_space=pltpu.VMEM)
    left_out, bond_out = pl.pallas_call(
        kernel,
        out_shape=(
            pltpu.VMEM((2,) + block, f32),
            pltpu.VMEM(block, f32),
        ),
        in_specs=[pl.BlockSpec(memory_space=pltpu.HBM)] * 4,
        out_specs=(inside, inside),
        scratch_shapes=[
            pltpu.SMEM(sector_size.shape, jnp.int32),
            pltpu.VMEM((2,) + block, f32),
            pltpu.VMEM(triangle, f32),
            pltpu.VMEM(triangle, f32),
            pltpu.VMEM((channels,) + block, f32),
            pltpu.VMEM((channels,) + block, f32),
            pltpu.VMEM((2, channels) + block, bf16),
            pltpu.VMEM((2, channels) + block, bf16),
            pltpu.VMEM((states, 2 * states), f32),
            pltpu.VMEM((states, 2 * states), f32),
            pltpu.VMEM(triangle, f32),
            pltpu.VMEM((2,) + triangle, f32),
            pltpu.VMEM((states // 2, states), f32),
            pltpu.VMEM((states // 2, states), f32),
            pltpu.VMEM(block, f32),
            pltpu.VMEM(block, f32),
            pltpu.VMEM((2,) + block, f32),
            pltpu.VMEM(block, f32),
            pltpu.VMEM((3, 2) + block, bf16),
            pltpu.VMEM((2, count - 1, 2, 128), f32),
            pltpu.VMEM((2, 2, 128), f32),
            pltpu.VMEM((EARLY,) + block, f32),
            pltpu.SemaphoreType.DMA((4,)),
            pltpu.SemaphoreType.DMA((8,)),
            pltpu.SemaphoreType.DMA((12,)),
            pltpu.SemaphoreType.DMA((2,)),
            pltpu.SemaphoreType.DMA((2,)),
            pltpu.SemaphoreType.DMA((EARLY,)),
            pltpu.SemaphoreType.DMA((EARLY,)),
            pltpu.SemaphoreType.REGULAR(((count - 1).bit_length(),)),
            pltpu.SemaphoreType.REGULAR,
        ],
        compiler_params=pltpu.CompilerParams(
            collective_id=0, has_side_effects=True, vmem_limit_bytes=60 * 1024 * 1024
        ),
        name="bond_update",
    )(sector_size, site_tensor, left_env, right_env)
    return pl.pallas_call(
        write_out,
        out_shape=(
            jax.ShapeDtypeStruct(site_tensor.shape, f32),
            jax.ShapeDtypeStruct((1,) + block, f32),
        ),
        in_specs=[inside, inside],
        out_specs=(anywhere, anywhere),
        scratch_shapes=[pltpu.SemaphoreType.DMA((2,))],
        compiler_params=pltpu.CompilerParams(vmem_limit_bytes=4 * 1024 * 1024),
        name="write_out",
    )(left_out, bond_out)


def solution(mesh):
    placed = (
        P(("real", "row"), None, None, None),
        P(("real", "row"), None, None, None),
        P(("real", "row"), None, None, None),
        P("real"),
    )
    return jax.shard_map(
        on_device,
        mesh=mesh,
        in_specs=placed,
        out_specs=(P(("real", "row"), None, None, None), P(("real", "row"), None, None)),
        check_vma=False,
    )
```

```python
import jax
import jax.numpy as jnp
from jax import lax
from jax.experimental import pallas as pl
from jax.experimental.pallas import tpu as pltpu
from jax.sharding import PartitionSpec as P

SIDE = 4
EARLY = 3
QUAD = 4
PANEL = 16
TAU = 0.15
highest = lax.Precision.HIGHEST
f32 = jnp.float32
bf16 = jnp.bfloat16
MESH = pl.DeviceIdType.MESH


def dot(a, b):
    return jnp.dot(a, b, preferred_element_type=f32)


def exact_dot(a, b, dims):
    return lax.dot_general(a, b, (dims, ((), ())), precision=highest, preferred_element_type=f32)


def split_2(value):
    high = value.astype(bf16)
    return high, (value - high.astype(f32)).astype(bf16)


def split_3(value):
    high = value.astype(bf16)
    rest = value - high.astype(f32)
    middle = rest.astype(bf16)
    return high, middle, (rest - middle.astype(f32)).astype(bf16)


def store_split(pair_ref, index, value):
    high, low = split_2(value)
    pair_ref[0, index] = high
    pair_ref[1, index] = low


def row_sum(value):
    rows, columns = value.shape
    summed = jnp.sum(value.reshape(rows // 8, 8, columns), axis=0)
    total = summed[:, :128]
    for start in range(128, columns, 128):
        total = total + summed[:, start : start + 128]
    return jnp.sum(total, axis=0, keepdims=True)


def square(top_left, top_right, bottom_left, bottom_right):
    top = jnp.concatenate([top_left, top_right], 1)
    return jnp.concatenate([top, jnp.concatenate([bottom_left, bottom_right], 1)], 0)


def panel_step(p, lo, hi, states, aug_ref, out_ref):
    base = pl.multiple_of(p * PANEL, PANEL)
    row_id = lax.broadcasted_iota(jnp.int32, (PANEL, 128), 0)
    offset = lax.rem(p * PANEL, 128)
    diag = aug_ref[pl.ds(base, PANEL), lo : lo + 128]
    diag = pltpu.roll(diag, lax.rem(128 - offset, 128), 1)
    columns = [jnp.broadcast_to(diag[:, r : r + 1], (PANEL, 128)) for r in range(PANEL)]
    tiles = [aug_ref[pl.ds(base, PANEL), t : t + 128] for t in range(lo, hi, 128)]
    scale = jnp.zeros((PANEL, 128), f32)
    for r in range(PANEL):
        inverse = lax.rsqrt(columns[r][r : r + 1, :])
        scale = jnp.where(row_id == r, inverse, scale)
        multiplier = columns[r] * inverse
        below = jnp.where(row_id > r, multiplier, 0.0)
        for s in range(r + 1, PANEL):
            columns[s] = columns[s] - below * multiplier[s : s + 1, :]
        if r < PANEL - 1:
            tiles = [tile - below * (tile[r : r + 1, :] * inverse) for tile in tiles]
    tiles = [tile * scale for tile in tiles]
    for t, tile in zip(range(lo, hi, 128), tiles):
        out_ref[pl.ds(base, PANEL), t : t + 128] = tile
    panel = jnp.concatenate(tiles, 1)
    q1, q2, q3 = split_3(panel)
    p1, p2, p3 = (q[:, : states - lo] for q in (q1, q2, q3))
    left = jnp.concatenate([p1, p1, p2, p2, p1, p3], 0)
    right = jnp.concatenate([q1, q2, q1, q2, q3, q1], 0)
    update = lax.dot_general(left, right, (((0,), (0,)), ((), ())), preferred_element_type=f32)
    aug_ref[lo:states, lo:hi] -= update


def kernel(
    size_hbm, site_hbm, left_hbm, right_hbm,
    left_out, bond_out,
    size_ref, site, gram_own, gram_in, left_f, right_f, left_s, right_s, aug, fac, bond_own, bond_in, inv_own, inv_in,
    bond, applied, applied_in, acc, field_s, red_in, red_own, relayed, prepared,
    local_sem, send_sem, recv_sem, red_send, red_recv, relay_send, relay_recv, greetings, go,
):
    count = lax.axis_size("row")
    me = lax.axis_index("row")
    states = site.shape[-1]
    half = states // 2
    channels = left_f.shape[0]
    moved = 2 * SIDE
    not_first, not_last = me > 0, me < count - 1
    to_right, to_left = jnp.minimum(me + 1, count - 1), jnp.maximum(me - 1, 0)

    loads = [
        pltpu.make_async_copy(site_hbm.at[0], site, local_sem.at[0]),
        pltpu.make_async_copy(left_hbm.at[0], left_f, local_sem.at[1]),
        pltpu.make_async_copy(right_hbm.at[0, moved:], right_f.at[moved:], local_sem.at[2]),
    ]
    load_size = pltpu.make_async_copy(size_hbm, size_ref, local_sem.at[3])
    load_size.start()
    for load in loads:
        load.start()

    quads = count // QUAD
    quad, place = me // QUAD, lax.rem(me, QUAD)
    goes_up, goes_down = 0 * quad, 0 * quad
    if count % QUAD == 0:
        goes_up = jnp.minimum(quad * SIDE // quads, EARLY)
        goes_down = jnp.minimum(SIDE - (quad + 1) * SIDE // quads, EARLY)
    relays_up, relays_down = place == QUAD - 1, place == 0
    paired = relays_up | relays_down if count % QUAD == 0 else me < 0
    across = jnp.clip(jnp.where(relays_up, me - QUAD + 1, me + QUAD - 1), 0, count - 1)
    frees = ((place == 1) & (me + QUAD - 1 < count), (place == 2) & (me >= QUAD - 1))
    over = (jnp.minimum(me + QUAD - 1, count - 1), jnp.maximum(me - QUAD + 1, 0))

    barrier = pltpu.get_barrier_semaphore()

    def greet(semaphore, distance):
        for there, peer in ((me >= distance, me - distance), (me < count - distance, me + distance)):

            @pl.when(there)
            def _():
                pl.semaphore_signal(semaphore, inc=1, device_id={"row": peer}, device_id_type=MESH)

    def greeted(semaphore, distance, more=0):
        peers_of = jnp.where(me >= distance, 1, 0) + jnp.where(me < count - distance, 1, 0)
        pl.semaphore_wait(semaphore, peers_of + more)

    levels = (count - 1).bit_length()

    def know(level):
        greeted(greetings.at[level], 2**level)
        if level + 1 < levels:
            greet(greetings.at[level + 1], 2 ** (level + 1))

    greet(barrier, 1)

    @pl.when(paired)
    def _():
        pl.semaphore_signal(barrier, inc=1, device_id={"row": across}, device_id_type=MESH)


    def remote(source, target, sent, received, peer):
        return pltpu.make_async_remote_copy(
            src_ref=source, dst_ref=target, send_sem=send_sem.at[sent], recv_sem=recv_sem.at[received],
            device_id={"row": peer}, device_id_type=MESH,
        )

    halves = [slice(0, half), slice(half, states)]
    peers = (to_right, to_left)

    def block_copy(side, k, peer):
        a = side * SIDE + k
        return remote(right_hbm.at[0, a], right_f.at[a], 1 + side, 1 + side, peer)

    def late_copy(side, part, peer):
        a, rows = side * SIDE + EARLY, halves[part]
        return remote(right_hbm.at[0, a, rows], right_f.at[a, rows], 8 + 2 * side + part, 3 + side, peer)

    def late_block(side):
        a = side * SIDE + EARLY
        return remote(right_hbm.at[0, a], right_f.at[a], 8 + 2 * side, 3 + side, to_right)

    def early_blocks(side):
        channels_of = pl.ds(side * SIDE, EARLY)
        return remote(right_hbm.at[0, channels_of], right_f.at[channels_of], 1 + side, 1 + side, to_right)

    def bond_copy(side, peer):
        return remote(bond_own, bond_in.at[side], 3 + side, 5 + side, peer)

    def applied_copy(side, part, peer):
        rows = halves[part]
        return remote(applied.at[rows], applied_in.at[side, rows], 5 + side, 7 + 2 * side + part, peer)

    def applied_sent(side):
        return remote(applied, applied_in.at[side], 5 + side, 7 + 2 * side, to_right)

    by_relay = (jnp.where(relays_up, goes_down, 0), jnp.where(relays_down, goes_up, 0))
    relay_amount = jnp.where(relays_up, goes_up, jnp.where(relays_down, goes_down, 0))
    beyond = jnp.clip(jnp.where(relays_up, me - QUAD, me + QUAD), 0, count - 1)
    relay_side = jnp.where(relays_up, 1, 0)

    def to_relay(side, k):
        return pltpu.make_async_remote_copy(
            src_ref=right_hbm.at[0, side * SIDE + k], dst_ref=relayed.at[k],
            send_sem=send_sem.at[1 + side], recv_sem=relay_recv.at[k],
            device_id={"row": across}, device_id_type=MESH,
        )

    def from_relay(k):
        return pltpu.make_async_remote_copy(
            src_ref=relayed.at[k], dst_ref=right_f.at[relay_side * SIDE + k],
            send_sem=relay_send.at[k], recv_sem=recv_sem.at[1 + relay_side],
            device_id={"row": beyond}, device_id_type=MESH,
        )

    def start_relayed(side):
        for k in range(EARLY):

            @pl.when(k < by_relay[side])
            def _():
                to_relay(side, k).start()

    def start_early(side):
        for k in range(EARLY):

            @pl.when(k >= by_relay[side])
            def _():
                sends[side][k].start()

    send_gram = remote(gram_own, gram_in, 0, 0, to_right)
    send_inv = remote(inv_own, inv_in, 7, 11, to_left)
    sends = [[block_copy(s, k, peers[s]) for k in range(EARLY)] for s in range(2)]
    send_late = [[late_copy(s, part, peers[s]) for part in range(2)] for s in range(2)]
    send_bond = [bond_copy(s, peers[s]) for s in range(2)]
    send_applied = [[applied_copy(s, part, peers[s]) for part in range(2)] for s in range(2)]

    load_size.wait()
    size = size_ref[me]
    size_before = size_ref[to_left]
    size_after = size_ref[to_right]
    row = lax.broadcasted_iota(jnp.int32, (states, states), 0)
    column = lax.broadcasted_iota(jnp.int32, (states, states), 1)
    block_row, block_column = row[:half, :half], column[:half, :half]
    on_diagonal = block_row == block_column
    live_pair = (row < size) & (column < size)

    @pl.when(me == 0)
    def _():
        gram_in[...] = jnp.zeros_like(gram_in)
        right_f[:SIDE] = jnp.zeros((SIDE, states, states), f32)
        bond_in[0] = jnp.zeros(bond_in.shape[1:], f32)
        applied_in[0] = jnp.zeros((states, states), f32)

    @pl.when(me == count - 1)
    def _():
        right_f[SIDE:moved] = jnp.zeros((SIDE, states, states), f32)
        bond_in[1] = jnp.zeros(bond_in.shape[1:], f32)
        applied_in[1] = jnp.zeros((states, states), f32)
        inv_in[...] = jnp.zeros_like(inv_in)

    def diagonal_rows(block):
        values = jnp.sum(jnp.where(on_diagonal, block, 0.0), axis=0, keepdims=True)
        return jnp.broadcast_to(values, (8, half))

    def store_packed(packed_ref, block, right_block, diagonal):
        packed_ref[:half, :half] = block
        packed_ref[:half, half:] = right_block
        packed_ref[half:, :half] = diagonal
        packed_ref[half:, half:] = diagonal

    loads[0].wait()
    gram_dims = ((0,), (0,))
    outer = jnp.where((row < size) & (column < size_after), site[1], 0.0)
    gram = exact_dot(outer, outer, gram_dims)
    store_packed(
        gram_own, jnp.where(block_column >= block_row, gram[:half, :half], gram[half:, half:]),
        gram[:half, half:], diagonal_rows(gram[half:, half:]),
    )
    greeted(barrier, 1, jnp.where(paired, 1, 0))
    greet(greetings.at[0], 1)
    start_relayed(0)

    waits_down, waits_up = not_last & (place == 1), not_first & (place == 2)

    @pl.when(not_last)
    def _():
        send_gram.start()

    @pl.when(not_last & ~waits_down)
    def _():
        start_early(0)

    upper = jnp.where(live_pair, site[0], 0.0)
    site[0] = upper
    gram = exact_dot(upper, upper, gram_dims)
    gram = gram + jnp.where((row == column) & (row >= size), 1.0, 0.0)
    aug[:, states:] = jnp.where(row == column, 1.0, 0.0).astype(f32)
    fac[...] = jnp.zeros_like(fac)
    start_relayed(1)

    @pl.when(not_first & ~waits_up)
    def _():
        start_early(1)

    know(0)

    @pl.when(not_first)
    def _():
        send_gram.wait_recv()

    know(1)
    block = gram_in[:half, :half]
    mirrored = block.T
    top_left = jnp.where(block_column >= block_row, block, mirrored)
    bottom_right = jnp.where(block_column < block_row, block, jnp.where(on_diagonal, gram_in[half : half + 1, :half], mirrored))
    aug[:half, :half] = gram[:half, :half] + top_left
    aug[:half, half:states] = gram[:half, half:] + gram_in[:half, half:]
    aug[half:, :half] = gram[half:, :half]
    aug[half:, half:states] = gram[half:, half:] + bottom_right
    loads[1].wait()
    loads[2].wait()

    panels = half // PANEL

    def first_half(p, carry):
        panel_step(p, 0, states + half, states, aug, fac)
        store_split(left_s, p, left_f[p])
        return carry

    def second_half(p, carry):
        panel_step(p, half, 2 * states, states, aug, fac)
        other = jnp.minimum(p, channels - 1)
        store_split(left_s, other, left_f[other])
        mine = jnp.minimum(p - panels + moved, channels - 1)
        store_split(right_s, mine, right_f[mine])
        return carry

    lax.fori_loop(0, panels // 2, first_half, 0)

    @pl.when(waits_down)
    def _():
        start_early(0)

    @pl.when(waits_up)
    def _():
        start_early(1)

    lax.fori_loop(panels // 2, panels, first_half, 0)
    know(2)
    lax.fori_loop(panels, 2 * panels, second_half, 0)
    for level in range(3, levels):
        know(level)

    bottom_right = fac[half:, half:states]
    store_packed(
        bond_own, jnp.where(block_column >= block_row, fac[:half, :half], bottom_right.T),
        fac[:half, half:states], diagonal_rows(bottom_right),
    )

    @pl.when(not_last)
    def _():
        for one in [send_bond[0]] + send_late[0]:
            one.start()

    @pl.when(not_first)
    def _():
        for one in [send_bond[1]] + send_late[1]:
            one.start()

    bond[...] = jnp.where(live_pair & (column >= row), fac[:, :states], 0.0)

    def relay(start, stop):
        for k in range(start, stop):

            @pl.when(k < relay_amount)
            def _():
                to_relay(0, k).wait_recv()
                from_relay(k).start()

    relay(0, 2)

    def put_field(which, value):
        field_s[which, 0], field_s[which, 1] = split_2(value)

    def middle_of(which, a, rows):
        high, low_part = field_s[which, 0, rows], field_s[which, 1, rows]
        r_high, r_low = right_s[0, a], right_s[1, a]
        return split_2(dot(high, r_high) + dot(high, r_low) + dot(low_part, r_high))

    def outside(total, l_high, l_low, m_high, m_low):
        return total + dot(l_high, m_high) + dot(l_high, m_low) + dot(l_low, m_high)

    def add_terms(total, which, a):
        m_high, m_low = middle_of(which, a, slice(None))
        return outside(total, left_s[0, a], left_s[1, a], m_high, m_low)

    def add_range(which, start, amount):
        group = next(n for n in (3, 2, 1) if amount % n == 0)

        def some(g, carry):
            total = acc[...]
            for k in range(group):
                total = add_terms(total, which, start + g * group + k)
            acc[...] = total
            return carry

        lax.fori_loop(0, amount // group, some, 0)

    near = 1 - lax.rem(me, 2)
    has_side = [jnp.where(s == 0, not_first, not_last) for s in (near, 1 - near)]
    sides = list(zip((near, 1 - near), has_side))

    acc[...] = jnp.zeros_like(acc)
    put_field(0, bond[...])
    add_range(0, moved, channels - moved)
    relay(2, EARLY)
    inverse = jnp.where(column <= row, fac[:, states:], 0.0)
    turned = ((1,), (1,))
    left_out[0] = exact_dot(site[0], inverse, turned)
    inv_own[:, :half] = jnp.where(block_column < block_row, inverse[:half, :half], inverse[half:, half:].T)
    inv_own[:, half:] = inverse[half:, :half]

    for order, (side, there) in enumerate(sides):
        if order == 1:
            for s in range(2):

                @pl.when(frees[s])
                def _():
                    early_blocks(s).wait_send()
                    send_late[s][0].wait_send()
                    pl.semaphore_signal(go, inc=1, device_id={"row": over[s]}, device_id_type=MESH)


        @pl.when(there)
        def _():
            bond_copy(side, to_right).wait_recv()

        limit = jnp.where(side == 0, size_before, size_after)
        block = bond_in[side, :half, :half]
        top_left = jnp.where(block_column >= block_row, block, 0.0)
        bottom_right = jnp.where(block_column > block_row, block.T, jnp.where(on_diagonal, bond_in[side, half : half + 1, :half], 0.0))
        field = square(top_left, bond_in[side, :half, half:], jnp.zeros((half, half), f32), bottom_right)
        put_field(1 + side, jnp.where((row < limit) & (column < limit), field, 0.0))

        @pl.when(there)
        def _():
            early_blocks(side).wait_recv()

        for k in range(EARLY):
            store_split(right_s, side * SIDE + k, right_f[side * SIDE + k])
        total = acc[...]
        for k in range(EARLY):
            total = add_terms(total, 1 + side, side * SIDE + k)
        acc[...] = total

        @pl.when(there)
        def _():
            late_block(side).wait_recv()

        last = side * SIDE + EARLY
        store_split(right_s, last, right_f[last])
        if order == 0:
            acc[...] = add_terms(acc[...], 1 + side, last)

    def reductions(t):
        for step in range(1, count):
            peer = lax.rem(me + step, count)
            yield pltpu.make_async_remote_copy(
                src_ref=red_own.at[t], dst_ref=red_in.at[t, step - 1],
                send_sem=red_send.at[t], recv_sem=red_recv.at[t],
                device_id={"row": peer}, device_id_type=MESH,
            )

    def all_reductions(t):
        return pltpu.make_async_remote_copy(
            src_ref=red_in.at[t], dst_ref=red_in.at[t], send_sem=red_send.at[t], recv_sem=red_recv.at[t],
            device_id={"row": to_right}, device_id_type=MESH,
        )

    held = (not_last & (place == QUAD - 1), not_first & (place == 0))
    last = (1 - near) * SIDE + EARLY
    m_high, m_low = middle_of(2 - near, last, slice(None))
    for part, rows in enumerate(halves):
        value = outside(acc[rows], left_s[0, last, rows], left_s[1, last, rows], m_high, m_low)
        applied[rows] = jnp.where(live_pair[rows], value, 0.0)
        if part == 1:
            red_own[0, :1] = row_sum(bond[...] * bond[...])
            red_own[0, 1:] = row_sum(bond[...] * applied[...])
            for one in reductions(0):
                one.start()

        @pl.when(not_last & ~held[0])
        def _():
            send_applied[0][part].start()

        @pl.when(not_first & ~held[1])
        def _():
            send_applied[1][part].start()

    @pl.when(not_first & ~held[1])
    def _():
        send_inv.start()

    for s in range(2):

        @pl.when(held[s])
        def _():
            pl.semaphore_wait(go, 1)
            for one in send_applied[s]:
                one.start()

    acc[...] = jnp.zeros_like(acc)
    put_field(0, applied[...])
    add_range(0, moved, channels - moved)

    def collect(t):
        all_reductions(t).wait_recv()
        return jnp.sum(red_own[t] + jnp.sum(red_in[t], axis=0), axis=1, keepdims=True)

    def prepare():
        total = collect(0)
        start_norm, energy = total[:1], total[1:] / total[:1]
        shifted = applied[...] - energy * bond[...]
        prepared[...] = bond[...] + TAU * shifted - (0.5 * TAU * TAU) * energy * (applied[...] + shifted)
        return start_norm

    for order, (side, there) in enumerate(sides):
        for part, rows in enumerate(halves):
            if order == 1 and part == 1:
                start_norm = prepare()

            @pl.when(there)
            def _():
                applied_copy(side, part, to_right).wait_recv()

            which = 1 + side
            field_s[which, 0, rows], field_s[which, 1, rows] = split_2(applied_in[side, rows])
            middles = [middle_of(which, side * SIDE + k, rows) for k in range(SIDE)]
            total = acc[...]
            for k in range(0, SIDE, 2):
                pair = [side * SIDE + k, side * SIDE + k + 1]
                l_high, l_low = (jnp.concatenate([left_s[i, a, :, rows] for a in pair], 1) for i in range(2))
                m_high, m_low = (jnp.concatenate([middles[k + j][i] for j in range(2)], 0) for i in range(2))
                total = outside(total, l_high, l_low, m_high, m_low)
            acc[...] = total

    acc[...] = prepared[...] + (0.5 * TAU * TAU) * jnp.where(live_pair, acc[...], 0.0)
    red_own[1, :1] = row_sum(acc[...] * acc[...])
    red_own[1, 1:] = jnp.zeros((1, 128), f32)
    for one in reductions(1):
        one.start()

    @pl.when(held[1])
    def _():
        send_inv.start()


    @pl.when(not_last)
    def _():
        send_inv.wait_recv()

    block = inv_in[:, :half]
    near_block, near_low = bond_in[1, :half, :half], bond_in[1, half : half + 1, :half]
    zeros = jnp.zeros((half, half), f32)
    top_left = jnp.where(block_column < block_row, block, jnp.where(on_diagonal, 1.0 / near_block, 0.0))
    bottom_right = jnp.where(block_column < block_row, block.T, jnp.where(on_diagonal, 1.0 / near_low, 0.0))
    outer = jnp.where((row < size) & (column < size_after), site[1], 0.0)
    outer = exact_dot(outer, square(top_left, zeros, inv_in[:, half:], bottom_right), turned)
    left_out[1] = jnp.where(not_last, outer, 0.0)

    @pl.when(not_last)
    def _():
        for one in [send_gram, send_bond[0], applied_sent(0)]:
            one.wait_send()

    @pl.when(not_first)
    def _():
        for one in [send_bond[1], applied_sent(1), send_inv]:
            one.wait_send()

    for s, there in enumerate((not_last, not_first)):

        @pl.when(there)
        def _():
            send_late[s][1].wait_send()

        @pl.when(there & ~frees[s])
        def _():
            early_blocks(s).wait_send()
            send_late[s][0].wait_send()

    for k in range(EARLY):

        @pl.when(k < relay_amount)
        def _():
            from_relay(k).wait_send()

    final_norm = collect(1)[:1]
    bond_out[...] = acc[...] * jnp.sqrt(start_norm / final_norm)
    for t in range(2):
        all_reductions(t).wait_send()


def write_out(left, bond, left_hbm, bond_hbm, sem):
    stores = [
        pltpu.make_async_copy(left, left_hbm.at[0], sem.at[0]),
        pltpu.make_async_copy(bond, bond_hbm.at[0], sem.at[1]),
    ]
    for store in stores:
        store.start()
    for store in stores:
        store.wait()


def on_device(site_tensor, left_env, right_env, sector_size):
    states = site_tensor.shape[-1]
    channels = left_env.shape[1]
    count = lax.axis_size("row")
    block = (states, states)
    triangle = (states // 2 + 8, states)
    anywhere = pl.BlockSpec(memory_space=pl.ANY)
    inside = pl.BlockSpec(memory_space=pltpu.VMEM)
    left_out, bond_out = pl.pallas_call(
        kernel,
        out_shape=(
            pltpu.VMEM((2,) + block, f32),
            pltpu.VMEM(block, f32),
        ),
        in_specs=[pl.BlockSpec(memory_space=pltpu.HBM)] * 4,
        out_specs=(inside, inside),
        scratch_shapes=[
            pltpu.SMEM(sector_size.shape, jnp.int32),
            pltpu.VMEM((2,) + block, f32),
            pltpu.VMEM(triangle, f32),
            pltpu.VMEM(triangle, f32),
            pltpu.VMEM((channels,) + block, f32),
            pltpu.VMEM((channels,) + block, f32),
            pltpu.VMEM((2, channels) + block, bf16),
            pltpu.VMEM((2, channels) + block, bf16),
            pltpu.VMEM((states, 2 * states), f32),
            pltpu.VMEM((states, 2 * states), f32),
            pltpu.VMEM(triangle, f32),
            pltpu.VMEM((2,) + triangle, f32),
            pltpu.VMEM((states // 2, states), f32),
            pltpu.VMEM((states // 2, states), f32),
            pltpu.VMEM(block, f32),
            pltpu.VMEM(block, f32),
            pltpu.VMEM((2,) + block, f32),
            pltpu.VMEM(block, f32),
            pltpu.VMEM((3, 2) + block, bf16),
            pltpu.VMEM((2, count - 1, 2, 128), f32),
            pltpu.VMEM((2, 2, 128), f32),
            pltpu.VMEM((EARLY,) + block, f32),
            pltpu.VMEM(block, f32),
            pltpu.SemaphoreType.DMA((4,)),
            pltpu.SemaphoreType.DMA((12,)),
            pltpu.SemaphoreType.DMA((12,)),
            pltpu.SemaphoreType.DMA((2,)),
            pltpu.SemaphoreType.DMA((2,)),
            pltpu.SemaphoreType.DMA((EARLY,)),
            pltpu.SemaphoreType.DMA((EARLY,)),
            pltpu.SemaphoreType.REGULAR(((count - 1).bit_length(),)),
            pltpu.SemaphoreType.REGULAR,
        ],
        compiler_params=pltpu.CompilerParams(
            collective_id=0, has_side_effects=True, vmem_limit_bytes=60 * 1024 * 1024
        ),
        name="bond_update",
    )(sector_size, site_tensor, left_env, right_env)
    return pl.pallas_call(
        write_out,
        out_shape=(
            jax.ShapeDtypeStruct(site_tensor.shape, f32),
            jax.ShapeDtypeStruct((1,) + block, f32),
        ),
        in_specs=[inside, inside],
        out_specs=(anywhere, anywhere),
        scratch_shapes=[pltpu.SemaphoreType.DMA((2,))],
        compiler_params=pltpu.CompilerParams(vmem_limit_bytes=4 * 1024 * 1024),
        name="write_out",
    )(left_out, bond_out)


def solution(mesh):
    placed = (
        P(("real", "row"), None, None, None),
        P(("real", "row"), None, None, None),
        P(("real", "row"), None, None, None),
        P("real"),
    )
    return jax.shard_map(
        on_device,
        mesh=mesh,
        in_specs=placed,
        out_specs=(P(("real", "row"), None, None, None), P(("real", "row"), None, None)),
        check_vma=False,
    )
```

```python
import jax
import jax.numpy as jnp
from jax import lax
from jax.experimental import pallas as pl
from jax.experimental.pallas import tpu as pltpu
from jax.sharding import PartitionSpec as P

SIDE = 4
EARLY = 3
QUAD = 4
PANEL = 16
TAU = 0.15
highest = lax.Precision.HIGHEST
f32 = jnp.float32
bf16 = jnp.bfloat16
MESH = pl.DeviceIdType.MESH


def dot(a, b):
    return jnp.dot(a, b, preferred_element_type=f32)


def exact_dot(a, b, dims):
    return lax.dot_general(a, b, (dims, ((), ())), precision=highest, preferred_element_type=f32)


def split_2(value):
    high = value.astype(bf16)
    return high, (value - high.astype(f32)).astype(bf16)


def split_3(value):
    high = value.astype(bf16)
    rest = value - high.astype(f32)
    middle = rest.astype(bf16)
    return high, middle, (rest - middle.astype(f32)).astype(bf16)


def store_split(pair_ref, index, value):
    high, low = split_2(value)
    pair_ref[0, index] = high
    pair_ref[1, index] = low


def row_sum(value):
    rows, columns = value.shape
    summed = jnp.sum(value.reshape(rows // 8, 8, columns), axis=0)
    total = summed[:, :128]
    for start in range(128, columns, 128):
        total = total + summed[:, start : start + 128]
    return jnp.sum(total, axis=0, keepdims=True)


def square(top_left, top_right, bottom_left, bottom_right):
    top = jnp.concatenate([top_left, top_right], 1)
    return jnp.concatenate([top, jnp.concatenate([bottom_left, bottom_right], 1)], 0)


def panel_step(p, lo, hi, states, aug_ref, out_ref):
    base = pl.multiple_of(p * PANEL, PANEL)
    row_id = lax.broadcasted_iota(jnp.int32, (PANEL, 128), 0)
    offset = lax.rem(p * PANEL, 128)
    diag = aug_ref[pl.ds(base, PANEL), lo : lo + 128]
    diag = pltpu.roll(diag, lax.rem(128 - offset, 128), 1)
    columns = [jnp.broadcast_to(diag[:, r : r + 1], (PANEL, 128)) for r in range(PANEL)]
    tiles = [aug_ref[pl.ds(base, PANEL), t : t + 128] for t in range(lo, hi, 128)]
    scale = jnp.zeros((PANEL, 128), f32)
    for r in range(PANEL):
        inverse = lax.rsqrt(columns[r][r : r + 1, :])
        scale = jnp.where(row_id == r, inverse, scale)
        multiplier = columns[r] * inverse
        below = jnp.where(row_id > r, multiplier, 0.0)
        for s in range(r + 1, PANEL):
            columns[s] = columns[s] - below * multiplier[s : s + 1, :]
        if r < PANEL - 1:
            tiles = [tile - below * (tile[r : r + 1, :] * inverse) for tile in tiles]
    tiles = [tile * scale for tile in tiles]
    for t, tile in zip(range(lo, hi, 128), tiles):
        out_ref[pl.ds(base, PANEL), t : t + 128] = tile
    panel = jnp.concatenate(tiles, 1)
    q1, q2, q3 = split_3(panel)
    p1, p2, p3 = (q[:, : states - lo] for q in (q1, q2, q3))
    left = jnp.concatenate([p1, p1, p2, p2, p1, p3], 0)
    right = jnp.concatenate([q1, q2, q1, q2, q3, q1], 0)
    update = lax.dot_general(left, right, (((0,), (0,)), ((), ())), preferred_element_type=f32)
    aug_ref[lo:states, lo:hi] -= update


def kernel(
    size_hbm, site_hbm, left_hbm, right_hbm,
    left_out, bond_out,
    size_ref, site, gram_own, gram_in, left_f, right_f, left_s, right_s, aug, fac, bond_own, bond_in, inv_own, inv_in,
    bond, applied, applied_in, acc, field_s, red_in, red_own, relayed, prepared, twice,
    local_sem, send_sem, recv_sem, red_send, red_recv, relay_send, relay_recv, greetings, go,
):
    count = lax.axis_size("row")
    me = lax.axis_index("row")
    states = site.shape[-1]
    half = states // 2
    channels = left_f.shape[0]
    moved = 2 * SIDE
    not_first, not_last = me > 0, me < count - 1
    to_right, to_left = jnp.minimum(me + 1, count - 1), jnp.maximum(me - 1, 0)

    loads = [
        pltpu.make_async_copy(site_hbm.at[0], site, local_sem.at[0]),
        pltpu.make_async_copy(left_hbm.at[0], left_f, local_sem.at[1]),
        pltpu.make_async_copy(right_hbm.at[0, moved:], right_f.at[moved:], local_sem.at[2]),
    ]
    load_size = pltpu.make_async_copy(size_hbm, size_ref, local_sem.at[3])
    load_size.start()
    for load in loads:
        load.start()

    quads = count // QUAD
    quad, place = me // QUAD, lax.rem(me, QUAD)
    goes_up, goes_down = 0 * quad, 0 * quad
    if count % QUAD == 0:
        goes_up = jnp.minimum(quad * SIDE // quads, EARLY)
        goes_down = jnp.minimum(SIDE - (quad + 1) * SIDE // quads, EARLY)
    relays_up, relays_down = place == QUAD - 1, place == 0
    paired = relays_up | relays_down if count % QUAD == 0 else me < 0
    across = jnp.clip(jnp.where(relays_up, me - QUAD + 1, me + QUAD - 1), 0, count - 1)
    frees = ((place == 1) & (me + QUAD - 1 < count), (place == 2) & (me >= QUAD - 1))
    over = (jnp.minimum(me + QUAD - 1, count - 1), jnp.maximum(me - QUAD + 1, 0))

    barrier = pltpu.get_barrier_semaphore()

    def greet(semaphore, distance):
        for there, peer in ((me >= distance, me - distance), (me < count - distance, me + distance)):

            @pl.when(there)
            def _():
                pl.semaphore_signal(semaphore, inc=1, device_id={"row": peer}, device_id_type=MESH)

    def greeted(semaphore, distance, more=0):
        peers_of = jnp.where(me >= distance, 1, 0) + jnp.where(me < count - distance, 1, 0)
        pl.semaphore_wait(semaphore, peers_of + more)

    levels = (count - 1).bit_length()

    def know(level):
        greeted(greetings.at[level], 2**level)
        if level + 1 < levels:
            greet(greetings.at[level + 1], 2 ** (level + 1))

    greet(barrier, 1)

    @pl.when(paired)
    def _():
        pl.semaphore_signal(barrier, inc=1, device_id={"row": across}, device_id_type=MESH)


    def remote(source, target, sent, received, peer):
        return pltpu.make_async_remote_copy(
            src_ref=source, dst_ref=target, send_sem=send_sem.at[sent], recv_sem=recv_sem.at[received],
            device_id={"row": peer}, device_id_type=MESH,
        )

    halves = [slice(0, half), slice(half, states)]
    peers = (to_right, to_left)

    def block_copy(side, k, peer):
        a = side * SIDE + k
        return remote(right_hbm.at[0, a], right_f.at[a], 1 + side, 1 + side, peer)

    def late_copy(side, part, peer):
        a, rows = side * SIDE + EARLY, (slice(0, states // 4), slice(states // 4, states))[part]
        return remote(right_hbm.at[0, a, rows], right_f.at[a, rows], 8 + 2 * side + part, 3 + side, peer)

    def late_block(side):
        a = side * SIDE + EARLY
        return remote(right_hbm.at[0, a], right_f.at[a], 8 + 2 * side, 3 + side, to_right)

    def early_blocks(side):
        channels_of = pl.ds(side * SIDE, EARLY)
        return remote(right_hbm.at[0, channels_of], right_f.at[channels_of], 1 + side, 1 + side, to_right)

    def bond_copy(side, peer):
        return remote(bond_own, bond_in.at[side], 3 + side, 5 + side, peer)

    def applied_copy(side, part, peer):
        rows = halves[part]
        return remote(applied.at[rows], applied_in.at[side, rows], 5 + side, 7 + 2 * side + part, peer)

    def applied_sent(side):
        return remote(applied, applied_in.at[side], 5 + side, 7 + 2 * side, to_right)

    by_relay = (jnp.where(relays_up, goes_down, 0), jnp.where(relays_down, goes_up, 0))
    relay_amount = jnp.where(relays_up, goes_up, jnp.where(relays_down, goes_down, 0))
    beyond = jnp.clip(jnp.where(relays_up, me - QUAD, me + QUAD), 0, count - 1)
    relay_side = jnp.where(relays_up, 1, 0)

    def to_relay(side, k):
        return pltpu.make_async_remote_copy(
            src_ref=right_hbm.at[0, side * SIDE + k], dst_ref=relayed.at[k],
            send_sem=send_sem.at[1 + side], recv_sem=relay_recv.at[k],
            device_id={"row": across}, device_id_type=MESH,
        )

    def from_relay(k):
        return pltpu.make_async_remote_copy(
            src_ref=relayed.at[k], dst_ref=right_f.at[relay_side * SIDE + k],
            send_sem=relay_send.at[k], recv_sem=recv_sem.at[1 + relay_side],
            device_id={"row": beyond}, device_id_type=MESH,
        )

    def start_relayed(side):
        for k in range(EARLY):

            @pl.when(k < by_relay[side])
            def _():
                to_relay(side, k).start()

    def start_early(side):
        for k in range(EARLY):

            @pl.when(k >= by_relay[side])
            def _():
                sends[side][k].start()

    send_gram = remote(gram_own, gram_in, 0, 0, to_right)
    send_inv = remote(inv_own, inv_in, 7, 11, to_left)
    sends = [[block_copy(s, k, peers[s]) for k in range(EARLY)] for s in range(2)]
    send_late = [[late_copy(s, part, peers[s]) for part in range(2)] for s in range(2)]
    send_bond = [bond_copy(s, peers[s]) for s in range(2)]
    send_applied = [[applied_copy(s, part, peers[s]) for part in range(2)] for s in range(2)]

    load_size.wait()
    size = size_ref[me]
    size_before = size_ref[to_left]
    size_after = size_ref[to_right]
    row = lax.broadcasted_iota(jnp.int32, (states, states), 0)
    column = lax.broadcasted_iota(jnp.int32, (states, states), 1)
    block_row, block_column = row[:half, :half], column[:half, :half]
    on_diagonal = block_row == block_column
    live_pair = (row < size) & (column < size)

    @pl.when(me == 0)
    def _():
        gram_in[...] = jnp.zeros_like(gram_in)
        right_f[:SIDE] = jnp.zeros((SIDE, states, states), f32)
        bond_in[0] = jnp.zeros(bond_in.shape[1:], f32)
        applied_in[0] = jnp.zeros((states, states), f32)

    @pl.when(me == count - 1)
    def _():
        right_f[SIDE:moved] = jnp.zeros((SIDE, states, states), f32)
        bond_in[1] = jnp.zeros(bond_in.shape[1:], f32)
        applied_in[1] = jnp.zeros((states, states), f32)
        inv_in[...] = jnp.zeros_like(inv_in)

    def diagonal_rows(block):
        values = jnp.sum(jnp.where(on_diagonal, block, 0.0), axis=0, keepdims=True)
        return jnp.broadcast_to(values, (8, half))

    def store_packed(packed_ref, block, right_block, diagonal):
        packed_ref[:half, :half] = block
        packed_ref[:half, half:] = right_block
        packed_ref[half:, :half] = diagonal
        packed_ref[half:, half:] = diagonal

    loads[0].wait()
    gram_dims = ((0,), (0,))
    outer = jnp.where((row < size) & (column < size_after), site[1], 0.0)
    gram = exact_dot(outer, outer, gram_dims)
    store_packed(
        gram_own, jnp.where(block_column >= block_row, gram[:half, :half], gram[half:, half:]),
        gram[:half, half:], diagonal_rows(gram[half:, half:]),
    )
    greeted(barrier, 1, jnp.where(paired, 1, 0))
    greet(greetings.at[0], 1)
    start_relayed(0)

    waits_down, waits_up = not_last & (place == 1), not_first & (place == 2)

    @pl.when(not_last)
    def _():
        send_gram.start()

    @pl.when(not_last & ~waits_down)
    def _():
        start_early(0)

    upper = jnp.where(live_pair, site[0], 0.0)
    site[0] = upper
    gram = exact_dot(upper, upper, gram_dims)
    gram = gram + jnp.where((row == column) & (row >= size), 1.0, 0.0)
    aug[:, states:] = jnp.where(row == column, 1.0, 0.0).astype(f32)
    fac[...] = jnp.zeros_like(fac)
    start_relayed(1)

    @pl.when(not_first & ~waits_up)
    def _():
        start_early(1)

    know(0)

    @pl.when(not_first)
    def _():
        send_gram.wait_recv()

    know(1)
    block = gram_in[:half, :half]
    mirrored = block.T
    top_left = jnp.where(block_column >= block_row, block, mirrored)
    bottom_right = jnp.where(block_column < block_row, block, jnp.where(on_diagonal, gram_in[half : half + 1, :half], mirrored))
    aug[:half, :half] = gram[:half, :half] + top_left
    aug[:half, half:states] = gram[:half, half:] + gram_in[:half, half:]
    aug[half:, :half] = gram[half:, :half]
    aug[half:, half:states] = gram[half:, half:] + bottom_right
    loads[1].wait()
    loads[2].wait()

    panels = half // PANEL

    def first_half(p, carry):
        panel_step(p, 0, states + half, states, aug, fac)
        store_split(left_s, p, left_f[p])
        return carry

    def second_half(p, carry):
        panel_step(p, half, 2 * states, states, aug, fac)
        other = jnp.minimum(p, channels - 1)
        store_split(left_s, other, left_f[other])
        mine = jnp.minimum(p - panels + moved, channels - 1)
        store_split(right_s, mine, right_f[mine])
        return carry

    lax.fori_loop(0, panels // 2, first_half, 0)

    @pl.when(waits_down)
    def _():
        start_early(0)

    @pl.when(waits_up)
    def _():
        start_early(1)

    lax.fori_loop(panels // 2, panels, first_half, 0)
    know(2)
    lax.fori_loop(panels, 2 * panels, second_half, 0)
    for level in range(3, levels):
        know(level)

    bottom_right = fac[half:, half:states]
    store_packed(
        bond_own, jnp.where(block_column >= block_row, fac[:half, :half], bottom_right.T),
        fac[:half, half:states], diagonal_rows(bottom_right),
    )

    @pl.when(not_last)
    def _():
        for one in [send_bond[0]] + send_late[0]:
            one.start()

    @pl.when(not_first)
    def _():
        for one in [send_bond[1]] + send_late[1]:
            one.start()

    bond[...] = jnp.where(live_pair & (column >= row), fac[:, :states], 0.0)

    def relay(start, stop):
        for k in range(start, stop):

            @pl.when(k < relay_amount)
            def _():
                to_relay(0, k).wait_recv()
                from_relay(k).start()

    relay(0, 2)

    def put_field(which, value):
        field_s[which, 0], field_s[which, 1] = split_2(value)

    def middle_of(which, a, rows):
        high, low_part = field_s[which, 0, rows], field_s[which, 1, rows]
        r_high, r_low = right_s[0, a], right_s[1, a]
        return split_2(dot(high, r_high) + dot(high, r_low) + dot(low_part, r_high))

    def outside(total, l_high, l_low, m_high, m_low):
        return total + dot(l_high, m_high) + dot(l_high, m_low) + dot(l_low, m_high)

    def add_terms(total, which, a):
        m_high, m_low = middle_of(which, a, slice(None))
        return outside(total, left_s[0, a], left_s[1, a], m_high, m_low)

    def add_range(target, which, start, amount):
        group = next(n for n in (3, 2, 1) if amount % n == 0)

        def some(g, carry):
            total = target[...]
            for k in range(group):
                total = add_terms(total, which, start + g * group + k)
            target[...] = total
            return carry

        lax.fori_loop(0, amount // group, some, 0)

    def side_half(side, there, part):
        rows, which = halves[part], 1 + side

        @pl.when(there)
        def _():
            applied_copy(side, part, to_right).wait_recv()

        field_s[which, 0, rows], field_s[which, 1, rows] = split_2(applied_in[side, rows])
        middles = [middle_of(which, side * SIDE + k, rows) for k in range(SIDE)]
        total = twice[...]
        for k in range(0, SIDE, 2):
            pair = [side * SIDE + k, side * SIDE + k + 1]
            l_high, l_low = (jnp.concatenate([left_s[i, a, :, rows] for a in pair], 1) for i in range(2))
            m_high, m_low = (jnp.concatenate([middles[k + j][i] for j in range(2)], 0) for i in range(2))
            total = outside(total, l_high, l_low, m_high, m_low)
        twice[...] = total

    near_first = place == 1 if count % QUAD == 0 else me < 0

    near = 1 - lax.rem(me, 2)
    has_side = [jnp.where(s == 0, not_first, not_last) for s in (near, 1 - near)]
    sides = list(zip((near, 1 - near), has_side))

    acc[...] = jnp.zeros_like(acc)
    twice[...] = jnp.zeros_like(twice)
    put_field(0, bond[...])
    add_range(acc, 0, moved, channels - moved)
    relay(2, EARLY)
    inverse = jnp.where(column <= row, fac[:, states:], 0.0)
    turned = ((1,), (1,))
    left_out[0] = exact_dot(site[0], inverse, turned)
    inv_own[:, :half] = jnp.where(block_column < block_row, inverse[:half, :half], inverse[half:, half:].T)
    inv_own[:, half:] = inverse[half:, :half]

    for order, (side, there) in enumerate(sides):
        if order == 1:
            for s in range(2):

                @pl.when(frees[s])
                def _():
                    early_blocks(s).wait_send()
                    send_late[s][0].wait_send()
                    pl.semaphore_signal(go, inc=1, device_id={"row": over[s]}, device_id_type=MESH)


        @pl.when(there)
        def _():
            bond_copy(side, to_right).wait_recv()

        limit = jnp.where(side == 0, size_before, size_after)
        block = bond_in[side, :half, :half]
        top_left = jnp.where(block_column >= block_row, block, 0.0)
        bottom_right = jnp.where(block_column > block_row, block.T, jnp.where(on_diagonal, bond_in[side, half : half + 1, :half], 0.0))
        field = square(top_left, bond_in[side, :half, half:], jnp.zeros((half, half), f32), bottom_right)
        put_field(1 + side, jnp.where((row < limit) & (column < limit), field, 0.0))

        @pl.when(there)
        def _():
            early_blocks(side).wait_recv()

        for k in range(EARLY):
            store_split(right_s, side * SIDE + k, right_f[side * SIDE + k])
        total = acc[...]
        for k in range(EARLY):
            total = add_terms(total, 1 + side, side * SIDE + k)
        acc[...] = total
        if order == 1:

            @pl.when(near_first)
            def _():
                for part in range(2):
                    side_half(near, has_side[0], part)


        @pl.when(there)
        def _():
            late_block(side).wait_recv()

        last = side * SIDE + EARLY
        store_split(right_s, last, right_f[last])
        if order == 0:
            acc[...] = add_terms(acc[...], 1 + side, last)

    def reductions(t):
        for step in range(1, count):
            peer = lax.rem(me + step, count)
            yield pltpu.make_async_remote_copy(
                src_ref=red_own.at[t], dst_ref=red_in.at[t, step - 1],
                send_sem=red_send.at[t], recv_sem=red_recv.at[t],
                device_id={"row": peer}, device_id_type=MESH,
            )

    def all_reductions(t):
        return pltpu.make_async_remote_copy(
            src_ref=red_in.at[t], dst_ref=red_in.at[t], send_sem=red_send.at[t], recv_sem=red_recv.at[t],
            device_id={"row": to_right}, device_id_type=MESH,
        )

    held = (not_last & (place == QUAD - 1), not_first & (place == 0))
    last = (1 - near) * SIDE + EARLY
    m_high, m_low = middle_of(2 - near, last, slice(None))
    for part, rows in enumerate(halves):
        value = outside(acc[rows], left_s[0, last, rows], left_s[1, last, rows], m_high, m_low)
        applied[rows] = jnp.where(live_pair[rows], value, 0.0)
        if part == 1:
            red_own[0, :1] = row_sum(bond[...] * bond[...])
            red_own[0, 1:] = row_sum(bond[...] * applied[...])
            for one in reductions(0):
                one.start()

        @pl.when(not_last & ~held[0])
        def _():
            send_applied[0][part].start()

        @pl.when(not_first & ~held[1])
        def _():
            send_applied[1][part].start()

    @pl.when(not_first & ~held[1])
    def _():
        send_inv.start()

    for s in range(2):

        @pl.when(held[s])
        def _():
            pl.semaphore_wait(go, 1)
            for one in send_applied[s]:
                one.start()

    put_field(0, applied[...])
    add_range(twice, 0, moved, channels - moved)

    def collect(t):
        all_reductions(t).wait_recv()
        return jnp.sum(red_own[t] + jnp.sum(red_in[t], axis=0), axis=1, keepdims=True)

    def prepare():
        total = collect(0)
        start_norm, energy = total[:1], total[1:] / total[:1]
        shifted = applied[...] - energy * bond[...]
        prepared[...] = bond[...] + TAU * shifted - (0.5 * TAU * TAU) * energy * (applied[...] + shifted)
        return start_norm

    for order, (side, there) in enumerate(sides):
        for part, rows in enumerate(halves):
            if order == 1 and part == 1:
                start_norm = prepare()
            if order == 0:

                @pl.when(~near_first)
                def _():
                    side_half(side, there, part)

            else:
                side_half(side, there, part)

    acc[...] = prepared[...] + (0.5 * TAU * TAU) * jnp.where(live_pair, twice[...], 0.0)
    red_own[1, :1] = row_sum(acc[...] * acc[...])
    red_own[1, 1:] = jnp.zeros((1, 128), f32)
    for one in reductions(1):
        one.start()

    @pl.when(held[1])
    def _():
        send_inv.start()


    @pl.when(not_last)
    def _():
        send_inv.wait_recv()

    block = inv_in[:, :half]
    near_block, near_low = bond_in[1, :half, :half], bond_in[1, half : half + 1, :half]
    zeros = jnp.zeros((half, half), f32)
    top_left = jnp.where(block_column < block_row, block, jnp.where(on_diagonal, 1.0 / near_block, 0.0))
    bottom_right = jnp.where(block_column < block_row, block.T, jnp.where(on_diagonal, 1.0 / near_low, 0.0))
    outer = jnp.where((row < size) & (column < size_after), site[1], 0.0)
    outer = exact_dot(outer, square(top_left, zeros, inv_in[:, half:], bottom_right), turned)
    left_out[1] = jnp.where(not_last, outer, 0.0)

    @pl.when(not_last)
    def _():
        for one in [send_gram, send_bond[0], applied_sent(0)]:
            one.wait_send()

    @pl.when(not_first)
    def _():
        for one in [send_bond[1], applied_sent(1), send_inv]:
            one.wait_send()

    for s, there in enumerate((not_last, not_first)):

        @pl.when(there)
        def _():
            send_late[s][1].wait_send()

        @pl.when(there & ~frees[s])
        def _():
            early_blocks(s).wait_send()
            send_late[s][0].wait_send()

    for k in range(EARLY):

        @pl.when(k < relay_amount)
        def _():
            from_relay(k).wait_send()

    final_norm = collect(1)[:1]
    bond_out[...] = acc[...] * jnp.sqrt(start_norm / final_norm)
    for t in range(2):
        all_reductions(t).wait_send()


def write_out(left, bond, left_hbm, bond_hbm, sem):
    stores = [
        pltpu.make_async_copy(left, left_hbm.at[0], sem.at[0]),
        pltpu.make_async_copy(bond, bond_hbm.at[0], sem.at[1]),
    ]
    for store in stores:
        store.start()
    for store in stores:
        store.wait()


def on_device(site_tensor, left_env, right_env, sector_size):
    states = site_tensor.shape[-1]
    channels = left_env.shape[1]
    count = lax.axis_size("row")
    block = (states, states)
    triangle = (states // 2 + 8, states)
    anywhere = pl.BlockSpec(memory_space=pl.ANY)
    inside = pl.BlockSpec(memory_space=pltpu.VMEM)
    left_out, bond_out = pl.pallas_call(
        kernel,
        out_shape=(
            pltpu.VMEM((2,) + block, f32),
            pltpu.VMEM(block, f32),
        ),
        in_specs=[pl.BlockSpec(memory_space=pltpu.HBM)] * 4,
        out_specs=(inside, inside),
        scratch_shapes=[
            pltpu.SMEM(sector_size.shape, jnp.int32),
            pltpu.VMEM((2,) + block, f32),
            pltpu.VMEM(triangle, f32),
            pltpu.VMEM(triangle, f32),
            pltpu.VMEM((channels,) + block, f32),
            pltpu.VMEM((channels,) + block, f32),
            pltpu.VMEM((2, channels) + block, bf16),
            pltpu.VMEM((2, channels) + block, bf16),
            pltpu.VMEM((states, 2 * states), f32),
            pltpu.VMEM((states, 2 * states), f32),
            pltpu.VMEM(triangle, f32),
            pltpu.VMEM((2,) + triangle, f32),
            pltpu.VMEM((states // 2, states), f32),
            pltpu.VMEM((states // 2, states), f32),
            pltpu.VMEM(block, f32),
            pltpu.VMEM(block, f32),
            pltpu.VMEM((2,) + block, f32),
            pltpu.VMEM(block, f32),
            pltpu.VMEM((3, 2) + block, bf16),
            pltpu.VMEM((2, count - 1, 2, 128), f32),
            pltpu.VMEM((2, 2, 128), f32),
            pltpu.VMEM((EARLY,) + block, f32),
            pltpu.VMEM(block, f32),
            pltpu.VMEM(block, f32),
            pltpu.SemaphoreType.DMA((4,)),
            pltpu.SemaphoreType.DMA((12,)),
            pltpu.SemaphoreType.DMA((12,)),
            pltpu.SemaphoreType.DMA((2,)),
            pltpu.SemaphoreType.DMA((2,)),
            pltpu.SemaphoreType.DMA((EARLY,)),
            pltpu.SemaphoreType.DMA((EARLY,)),
            pltpu.SemaphoreType.REGULAR(((count - 1).bit_length(),)),
            pltpu.SemaphoreType.REGULAR,
        ],
        compiler_params=pltpu.CompilerParams(
            collective_id=0, has_side_effects=True, vmem_limit_bytes=60 * 1024 * 1024
        ),
        name="bond_update",
    )(sector_size, site_tensor, left_env, right_env)
    return pl.pallas_call(
        write_out,
        out_shape=(
            jax.ShapeDtypeStruct(site_tensor.shape, f32),
            jax.ShapeDtypeStruct((1,) + block, f32),
        ),
        in_specs=[inside, inside],
        out_specs=(anywhere, anywhere),
        scratch_shapes=[pltpu.SemaphoreType.DMA((2,))],
        compiler_params=pltpu.CompilerParams(vmem_limit_bytes=4 * 1024 * 1024),
        name="write_out",
    )(left_out, bond_out)


def solution(mesh):
    placed = (
        P(("real", "row"), None, None, None),
        P(("real", "row"), None, None, None),
        P(("real", "row"), None, None, None),
        P("real"),
    )
    return jax.shard_map(
        on_device,
        mesh=mesh,
        in_specs=placed,
        out_specs=(P(("real", "row"), None, None, None), P(("real", "row"), None, None)),
        check_vma=False,
    )
```
